32 devices in a mesh: fov: 8 (over z, x), row: 4 (over y, core).
Axes of the slice: x: 2, y: 2, z: 4, core: 2. Of those that a mesh axis runs over, the one named last changes fastest.
Arguments:
- frames: bfloat16 [8, 5, 512, 512], P('fov', None, 'row'), parts along dimension 0, may hold values from 0.01 to 13, as said below
- phase_offset: float32 [8], P('fov'), parts along dimension 0, may hold values from -3.140625 to 3.140625
- order_gain: float32 [8, 5], P('fov'), parts along dimension 0, may hold values from 0.5 to 2
- band_shift: int32 [8, 2], P('fov'), parts along dimension 0, may hold values from -96 to 96
Outputs:
- picture: float32 [8192, 1024], P(('fov', 'row')), parts along dimension 0
The draws below stay inside these ranges and needn't reach their ends.
There are 8 independent parts, one for each index of `fov`. The reference program is written for one: setup_inputs(seed, part) draws one part's arguments, and reference() takes and returns one part's arrays. A program takes and returns all parts, laid end to end along the dimension named above; each array names one. Nothing has to cross between parts.
Inputs may be any that keep to these rules, and one draw needn't show every extreme that they name: `frames`: positive intensities. `band_shift`: offsets in frequency bins of the 1024-point grid, row component first.
All inputs are finite; a program needn't handle non-finite values.
Results may differ from the reference program's by a relative error of at most 0.0003.
Values sent between devices are 32-bit elements; how exact they have to be, the bound alone decides.
A program may use at most 128 MiB of HBM per device.

```python
import math
import jax
import jax.numpy as jnp
from jax import lax

PIX = 512
GRID = 1024
PHASES = 5
ANGLES = 1


def draw_frames(key, part):
    subkeys = jax.random.split(key, 4)
    frame_shape = (ANGLES, PHASES, PIX, PIX)
    levels = jax.random.uniform(subkeys[0], (ANGLES, PHASES, 1, 1), jnp.float32, 0.5, 2.0)
    slopes = jax.random.uniform(subkeys[1], (ANGLES, PHASES, 1, 1), jnp.float32, 0.6, 1.2)
    signs_draw = jnp.where(jax.random.bernoulli(subkeys[2], 0.5, (ANGLES, PHASES, 1, 1)), 1.0, -1.0)
    row_pos = (jnp.arange(PIX, dtype=jnp.float32) / PIX - 0.5).reshape(1, 1, PIX, 1)
    profile = jnp.exp(2.0 * slopes * signs_draw * row_pos)
    texture = jnp.clip(1.0 + 0.3 * jax.random.normal(subkeys[3], frame_shape, jnp.float32), 0.1, 1.9)
    return (levels * profile * texture).astype(jnp.bfloat16)


def setup_inputs(seed: int = 0, part: int = 0) -> dict:
    seeds = jax.random.split(jax.random.key(seed), 5)
    own_keys = jax.random.split(jax.random.fold_in(seeds[4], part), 5)
    frames = draw_frames(jax.random.fold_in(jax.random.fold_in(seeds[4], part), 71), part)
    phase_offset = jnp.clip(jax.random.uniform(own_keys[1], (ANGLES,), jnp.float32, -3.140625, 3.140625), -3.140625, 3.140625)
    order_gain = jnp.clip(jnp.exp(jax.random.uniform(own_keys[2], (ANGLES, PHASES), jnp.float32, math.log(0.5), math.log(2.0))), 0.5, 2.0)
    band_shift = jax.random.randint(own_keys[3], (ANGLES, 2), -(3 * PIX) // 16, (3 * PIX) // 16 + 1).astype(jnp.int32)
    return {"frames": frames, "phase_offset": phase_offset, "order_gain": order_gain, "band_shift": band_shift}


wiener = 0.1
gain_out = 8.0
cut_share = 0.45

def wrap_signed(values, length):
    return (values + length // 2) % length - length // 2

def transfer_curve(freq_y, freq_x, cutoff):
    float_y = freq_y.astype(jnp.float32)
    float_x = freq_x.astype(jnp.float32)
    radius = jnp.sqrt(float_y * float_y + float_x * float_x) / cutoff
    radius = jnp.minimum(radius, 1.0)
    return 2.0 / math.pi * (jnp.arccos(radius) - radius * jnp.sqrt(1.0 - radius * radius))

def reference(frames, phase_offset, order_gain, band_shift):
    intensity = frames.astype(jnp.float32)
    totals = lax.optimization_barrier(jnp.sum(intensity, axis=(2, 3)))
    scales = PIX * PIX / totals
    half_pix = PIX // 2
    cutoff = cut_share * PIX
    signed_index = wrap_signed(jnp.arange(PIX, dtype=jnp.int32), PIX)
    base_curve = transfer_curve(signed_index[:, None], signed_index[None, :], cutoff)
    fine_index = jnp.arange(GRID, dtype=jnp.int32)
    numerator = None
    denominator = jnp.full((GRID, GRID), wiener, jnp.float32)
    for angle_idx in range(ANGLES):
        phase_angle = 2.0 * math.pi * jnp.arange(PHASES, dtype=jnp.float32) / PHASES + phase_offset[angle_idx]
        weight = scales[angle_idx] / PHASES
        shift_y = band_shift[angle_idx, 0]
        shift_x = band_shift[angle_idx, 1]
        for order_idx in range(PHASES):
            order_val = order_idx - PHASES // 2
            coef_re = weight * jnp.cos(order_val * phase_angle)
            coef_im = -weight * jnp.sin(order_val * phase_angle)
            band_re = jnp.tensordot(coef_re, intensity[angle_idx], axes=1, precision=lax.Precision.HIGHEST)
            band_im = jnp.tensordot(coef_im, intensity[angle_idx], axes=1, precision=lax.Precision.HIGHEST)
            gain_val = order_gain[angle_idx, order_idx]
            spectrum = jnp.fft.fft2(lax.complex(band_re, band_im)) * (gain_val * base_curve)
            zero_block = jnp.zeros_like(spectrum)
            tall = jnp.concatenate([spectrum[:half_pix], zero_block, spectrum[half_pix:]], axis=0)
            zero_wide = jnp.zeros_like(tall)
            embedded = jnp.concatenate([tall[:, :half_pix], zero_wide, tall[:, half_pix:]], axis=1)
            moved = jnp.roll(jnp.roll(embedded, order_val * shift_y, axis=0), order_val * shift_x, axis=1)
            numerator = moved if numerator is None else numerator + moved
            shifted_curve = transfer_curve(wrap_signed(fine_index[:, None] - order_val * shift_y, GRID), wrap_signed(fine_index[None, :] - order_val * shift_x, GRID), cutoff)
            denominator = denominator + gain_val * gain_val * shifted_curve * shifted_curve
    picture = jnp.fft.ifft2(numerator / denominator)
    return (gain_out * jnp.real(picture)).astype(jnp.float32)
```

```python
import functools
import math

import jax
import jax.numpy as jnp
import numpy as np
from jax import lax
from jax.experimental import pallas as pl
from jax.experimental.pallas import tpu as pltpu
from jax.sharding import PartitionSpec as P

MESH = pl.DeviceIdType.MESH
wiener = 0.1
gain_out = 8.0
cut_share = 0.45
CORES = 2
STEP = 16


def max_shift(pixels):
    return 3 * pixels // 16


def split_table(table):
    high = table.astype(np.float32).astype(jnp.bfloat16)
    low = (table - high.astype(np.float64)).astype(np.float32).astype(jnp.bfloat16)
    return np.stack([high, low])


def cos_sin(points, freqs, length):
    angle = 2.0 * math.pi * ((points[:, None] * freqs[None, :]) % length) / length
    return np.cos(angle), np.sin(angle)


def lane_order(wide):
    drop = wide // 4
    return np.concatenate([np.arange(1, drop + 1), [0], np.arange(drop + 1, wide)])


def tables(pixels, count):
    half = pixels // 2
    wide = half // CORES
    chips = count // CORES
    drop = wide // 4
    points = np.arange(pixels)
    freqs = np.arange(half)
    alternate = 1.0 - 2.0 * (points % 2)
    cos_f, sin_f = cos_sin(points, freqs, pixels)
    sin_f[:, 0] = alternate
    column = np.concatenate([cos_f, sin_f], axis=1).T
    column = column.reshape(pixels, chips, pixels // chips).transpose(1, 0, 2)
    inverse = []
    for odd in range(2):
        cos_i, sin_i = cos_sin(2 * points + odd, freqs, 2 * pixels)
        sin_i[:, 0] = alternate
        inverse.append(np.concatenate([cos_i, sin_i], axis=1))
    inverse = np.stack(inverse)
    lead, last = [], []
    places = np.arange(2 * pixels)
    for core in range(CORES):
        own = CORES * lane_order(wide) + core
        lead.append(np.concatenate([cos_f[:, own], sin_f[:, own]], axis=1))
        near_cos, near_sin = cos_sin(places, own, 2 * pixels)
        share = np.where(own == 0, 1.0, 2.0)
        near = np.concatenate([(near_cos * share).T, (-near_sin * share).T])
        mirror = np.where(own == 0, half, pixels - own)
        assert (pixels - own[:drop]).min() > cut_share * pixels + 2 * max_shift(pixels)
        far_cos, far_sin = cos_sin(places, mirror, 2 * pixels)
        keep = np.where(np.arange(wide) < drop, 0.0, 2.0)
        far = np.concatenate([(far_cos * keep).T, (-far_sin * keep).T])
        last.append(np.stack([near, far]))
    return tuple(split_table(t) for t in (np.stack(lead), column, inverse, np.stack(last)))


def otf_polynomial():
    nodes = 0.5 + 0.5 * np.cos(math.pi * (np.arange(64) + 0.5) / 64)
    nodes = np.minimum(nodes, 0.9985)
    root = np.sqrt(1 - nodes * nodes)
    values = 2 / math.pi * (np.arccos(nodes) - nodes * root) / root**3
    fit = np.polynomial.chebyshev.Chebyshev.fit(nodes, values, 9, domain=[0, 1])
    poly = fit.convert(kind=np.polynomial.Polynomial).coef
    return [float(c) for c in poly[::-1]]


def halves(value):
    high = value.astype(jnp.bfloat16)
    return high, (value - high.astype(jnp.float32)).astype(jnp.bfloat16)


def dot(left, right):
    return jnp.dot(left, right, preferred_element_type=jnp.float32)


def dot3(left_hi, left_lo, right_hi, right_lo):
    return dot(left_hi, right_hi) + (dot(left_hi, right_lo) + dot(left_lo, right_hi))


def kernel(count, poly, frames_h, offset, gain, shift, lead_h, column_h, inverse_h, last_h, out,
           frames, lead, column, inverse, last, tot_send, tot, planes, send1, recv1, mixed, alpha, coef,
           near_send, near, send_a, recv_a, send_b, recv_b, part, woven,
           frame_sem, table_sem, tot_ss, tot_rs, ss1, rs1, near_ss, near_rs, a_ss, a_rs, b_ss, b_rs):
    me = lax.axis_index("row")
    chips = count // CORES
    chip, core = me // CORES, me % CORES
    sib_core = 1 - core
    phases, rows, pixels = frames.shape
    half = pixels // 2
    wide = half // CORES
    drop = wide // 4
    orders = phases // 2
    mid = phases // 2
    others = [lax.rem(me + step, count) for step in range(1, count)]
    far_chips = [lax.rem(chip + step, chips) for step in range(1, chips)]
    sibling = chip * CORES + sib_core

    barrier = pltpu.get_barrier_semaphore()
    for peer in others:
        pl.semaphore_signal(barrier, inc=1, device_id={"row": peer}, device_id_type=MESH)
    frame_loads = []
    for p in range(phases):
        frame_loads.append(pltpu.make_async_copy(frames_h.at[0, p], frames.at[p], frame_sem.at[p]))
        frame_loads[p].start()
    loads = []
    for idx, (source, target) in enumerate(
        ((lead_h, lead), (column_h.at[:, chip], column), (inverse_h, inverse), (last_h, last))
    ):
        loads.append(pltpu.make_async_copy(source, target, table_sem.at[idx]))
    loads[0].start()

    lane8 = lax.broadcasted_iota(jnp.int32, (8, 128), 1)
    total_part = jnp.zeros((8, 128), jnp.float32)
    for p in range(phases):
        frame_loads[p].wait()
        f = frames[p].astype(jnp.float32)
        s = jnp.sum(jnp.sum(f, axis=0, keepdims=True), axis=1, keepdims=True)
        total_part = total_part + jnp.where(lane8 == p, s, 0.0)
    tot_send[...] = total_part
    tot[me] = total_part
    pl.semaphore_wait(barrier, count - 1)

    def tot_copy(peer, slot):
        return pltpu.make_async_remote_copy(
            src_ref=tot_send, dst_ref=tot.at[slot], send_sem=tot_ss.at[peer], recv_sem=tot_rs.at[slot],
            device_id={"row": peer}, device_id_type=MESH)

    for peer in others:
        tot_copy(peer, me).start()
    for load in loads[1:]:
        load.start()

    shift_y, shift_x = shift[0, 0], shift[0, 1]
    inv_cut = 1.0 / (cut_share * pixels)
    scale_out = 0.5 * gain_out / (4.0 * pixels * pixels)
    gains = [gain[0, j] for j in range(phases)]
    squares = [g * g for g in gains]
    scaled = [g * scale_out for g in gains]
    reach = int(cut_share * pixels) + 1 + 2 * max_shift(pixels)
    single = (pixels - reach) // STEP

    def own_freq(shape):
        lane = lax.broadcasted_iota(jnp.int32, shape, 1)
        place = jnp.where(lane < drop, lane + 1, jnp.where(lane == drop, 0, lane))
        return CORES * place + core

    def make_alpha(side):
        freq = own_freq((STEP, wide))
        if side:
            freq = jnp.where(freq == 0, half, pixels - freq)
        used = [j for j in range(phases) if not (side and j == mid)]
        sq_xs = {}
        for j in used:
            fx = (freq - (j - mid) * shift_x).astype(jnp.float32) * inv_cut
            sq_xs[j] = fx * fx + 1e-30
        offs = {j: ((j - mid) * shift_y).astype(jnp.float32) * inv_cut for j in used}

        def block(first, slots, top):
            row = first + lax.broadcasted_iota(jnp.int32, (STEP, wide), 0)
            for slot in slots:
                big_y = row if slot % 2 == 0 else -row
                if top and slot % 2:
                    big_y = jnp.where(row == 0, -half, big_y)
                if slot == 2:
                    big_y = big_y - pixels
                if slot == 3:
                    big_y = big_y + pixels
                unit_y = big_y.astype(jnp.float32) * inv_cut
                den = jnp.full((STEP, wide), wiener, jnp.float32)
                den_m = jnp.full((STEP, wide), wiener, jnp.float32)
                values = {}
                for j in used:
                    fy = unit_y - offs[j]
                    t = fy * fy + sq_xs[j]
                    r = t * lax.rsqrt(t)
                    u = jnp.maximum(1.0 - t, 1e-30)
                    v = u * lax.rsqrt(u)
                    acc = poly[0] * r + poly[1]
                    for c in poly[2:]:
                        acc = acc * r + c
                    value = acc * (u * v)
                    values[j] = value
                    sq = value * value
                    den = den + squares[j] * sq
                    den_m = den_m + squares[phases - 1 - j] * sq
                both = 1.0 / (den * den_m)
                inv, inv_m = den_m * both, den * both
                for j in used:
                    alpha[side, slot, j, pl.ds(first, STEP), :] = values[j] * (
                        scaled[j] * inv + scaled[phases - 1 - j] * inv_m)

        block(0, (0, 1, 2, 3), True)

        def few(i, carry):
            block(pl.multiple_of(i * STEP, STEP), (0, 1), False)
            return carry

        def many(i, carry):
            block(pl.multiple_of(i * STEP, STEP), (0, 1, 2, 3), False)
            return carry

        lax.fori_loop(1, max(single, 1), few, 0)
        lax.fori_loop(max(single, 1), half // STEP, many, 0)

    turn = 2.0 * math.pi / pixels

    def ramp(points, step):
        arg = ((points * step) & (pixels - 1)).astype(jnp.float32) * turn
        return jnp.cos(arg), jnp.sin(arg)

    def times(left, right):
        return left[0] * right[0] - left[1] * right[1], left[0] * right[1] + left[1] * right[0]

    row8 = lax.broadcasted_iota(jnp.int32, (8, 128), 0) + me * rows
    wave_x = [ramp(lane8 + 128 * k, shift_x) for k in range(pixels // 128)]
    base = ramp(row8, shift_y)
    leap = ramp(jnp.full((8, 128), 8, jnp.int32), shift_y)
    pieces = [base]
    for k in range(1, rows // 8):
        pieces.append(times(pieces[-1], leap))
    wave_y = tuple(jnp.concatenate([q[k] for q in pieces], axis=0) for k in range(2))
    waves = {1: (wave_y, wave_x)}
    for order in range(2, orders + 1):
        last_y, last_x = waves[order - 1]
        waves[order] = (times(last_y, wave_y), [times(a, b) for a, b in zip(last_x, wave_x)])
    angle = 2.0 * math.pi / phases * lane8.astype(jnp.float32) + offset[0]
    unmix = {order: (jnp.cos(order * angle), jnp.sin(order * angle)) for order in range(1, orders + 1)}

    make_alpha(0)

    for peer in others:
        tot_copy(peer, peer).wait_recv()
    total = tot[0]
    for d in range(1, count):
        total = total + tot[d]
    level = jnp.where(lane8 < phases, float(pixels * pixels), 0.0) / jnp.where(lane8 < phases, total, 1.0)
    level = level / phases

    groups = [(4 * g, 4, g + 1) for g in range(orders)] + [(4 * orders, 2, 0)]

    def send1_copy(slot_core, g):
        first, tiles, _ = groups[g]
        window = pl.ds(first * wide, tiles * wide)
        return pltpu.make_async_remote_copy(
            src_ref=send1.at[:, window],
            dst_ref=recv1.at[pl.ds(pl.multiple_of(slot_core * rows, rows), rows), window],
            send_sem=ss1.at[g], recv_sem=rs1.at[g],
            device_id={"row": sibling}, device_id_type=MESH)

    def spectrum_lines(g, place, target_core, write):
        first, tiles, order = groups[g]
        span = pl.ds(place * rows, (2 if order else 1) * rows)
        result = dot3(planes[0, span, :], planes[1, span, :], lead[0, target_core], lead[1, target_core])
        special = jnp.logical_and(
            lax.broadcasted_iota(jnp.int32, (rows, wide), 1) == drop, target_core == 0)
        if order:
            cr, sr = result[:rows, :wide], result[:rows, wide:]
            ci, si = result[rows:, :wide], result[rows:, wide:]
            values = [jnp.where(special, cr, cr + si), jnp.where(special, ci, ci - sr),
                      jnp.where(special, sr, cr - si), jnp.where(special, si, ci + sr)]
        else:
            values = [result[:, :wide], jnp.where(special, 0.0, -result[:, wide:])]
        for k, value in enumerate(values):
            write(pl.ds((first + k) * wide, wide), value)

    def write_send(window, value):
        send1[:, window] = value

    mine = pl.ds(pl.multiple_of(core * rows, rows), rows)

    def write_mine(window, value):
        recv1[mine, window] = value

    loads[0].wait()
    places = [2 * g if groups[g][2] else 2 * orders for g in range(len(groups))]
    for g, (first, tiles, order) in enumerate(groups):
        coef_re, coef_im = level, None
        if order:
            coef_re, coef_im = level * unmix[order][0], -level * unmix[order][1]
        for x in range(pixels // 128):
            span = pl.ds(x * 128, 128)
            bands = [None, None]
            for p in range(phases):
                f = frames[p, :, span].astype(jnp.float32)
                for k, coefs in enumerate((coef_re, coef_im)):
                    if coefs is None:
                        continue
                    term = coefs[:1, p:p + 1] * f
                    bands[k] = term if bands[k] is None else bands[k] + term
            if order:
                wy, wx = waves[order][0], waves[order][1][x]
                ramps = times(wy, (wx[0][:1], wx[1][:1]))
                bands = times(bands, ramps)
            for k, value in enumerate(bands[:2 if order else 1]):
                hi, lo = halves(value)
                planes[0, pl.ds((places[g] + k) * rows, rows), span] = hi
                planes[1, pl.ds((places[g] + k) * rows, rows), span] = lo
        spectrum_lines(g, places[g], sib_core, write_send)
        send1_copy(core, g).start()
    for g in range(len(groups)):
        spectrum_lines(g, places[g], core, write_mine)

    loads[1].wait()
    for g, (first, tiles, order) in enumerate(groups):
        window = pl.ds(first * wide, tiles * wide)
        send1_copy(sib_core, g).wait_recv()
        hi, lo = halves(recv1[:, window])
        mixed[:, window] = dot3(column[0], column[1], hi, lo)

    special = jnp.logical_and(lax.broadcasted_iota(jnp.int32, (STEP, wide), 1) == drop, core == 0)

    def combine(side):
        def block(first, second, top):
            here, below = pl.ds(first, STEP), pl.ds(half + first, STEP)
            row0 = None
            if top:
                row0 = lax.broadcasted_iota(jnp.int32, (STEP, wide), 0) == 0

            def pick(at_top, value):
                return jnp.where(row0, at_top, value) if top else value

            def signs(tile):
                re, im = pl.ds(tile * wide, wide), pl.ds((tile + 1) * wide, wide)
                cr, ci, sr, si = mixed[here, re], mixed[here, im], mixed[below, re], mixed[below, im]
                plus = (pick(cr, cr + si), pick(ci, ci - sr))
                minus = (pick(sr, cr - si), pick(si, ci + sr))
                return plus, minus

            slots = (0, 1, 2, 3) if second else (0, 1)
            sums = {slot: [None, None] for slot in slots}

            def add(slot, k, term):
                sums[slot][k] = term if sums[slot][k] is None else sums[slot][k] + term

            if side == 0:
                center = signs(4 * orders)
                for slot in slots:
                    a = alpha[side, slot, mid, here, :]
                    for k in range(2):
                        add(slot, k, a * center[slot % 2][k])
            for order in range(1, orders + 1):
                pos, neg = signs(4 * (order - 1)), signs(4 * (order - 1) + 2)
                direct, other = (pos, neg) if side == 0 else (neg, pos)
                partner = [[jnp.where(special, direct[s][k], other[s][k]) for k in range(2)] for s in range(2)]
                if top:
                    swap = [[pick(partner[s][k], partner[1 - s][k]) for k in range(2)] for s in range(2)]
                else:
                    swap = [partner[1], partner[0]]
                for slot in slots:
                    s = slot % 2
                    up, down = alpha[side, slot, mid + order, here, :], alpha[side, slot, mid - order, here, :]
                    add(slot, 0, up * direct[s][0] + down * swap[s][0])
                    add(slot, 1, up * direct[s][1] - down * swap[s][1])
            for a in range(2):
                def folded(s, k):
                    if not second:
                        return sums[s][k]
                    return sums[s][k] + sums[2 + s][k] if a == 0 else sums[s][k] - sums[2 + s][k]

                pr, pi, mr, mi = folded(0, 0), folded(0, 1), folded(1, 0), folded(1, 1)
                low_top = (mr, mi) if a == 0 else (mi, -mr)
                values = [(here, 0, pick(pr, pr + mr)), (here, 1, pick(pi, pi + mi)),
                          (below, 0, pick(low_top[0], mi - pi)), (below, 1, pick(low_top[1], pr - mr))]
                for place, k, value in values:
                    hi, lo = halves(value)
                    coef[0, side, a, place, pl.ds(k * wide, wide)] = hi
                    coef[1, side, a, place, pl.ds(k * wide, wide)] = lo

        block(0, True, True)

        def few(i, carry):
            block(pl.multiple_of(i * STEP, STEP), False, False)
            return carry

        def many(i, carry):
            block(pl.multiple_of(i * STEP, STEP), True, False)
            return carry

        lax.fori_loop(1, max(single, 1), few, 0)
        lax.fori_loop(max(single, 1), half // STEP, many, 0)

    def to_rows(side, a, first_row, length):
        t = pl.ds(pl.multiple_of(first_row, rows), length)
        return dot3(inverse[0, a, t, :], inverse[1, a, t, :], coef[0, side, a], coef[1, side, a])

    def a_copy(c, kc, slot_chip, slot_core, a):
        return pltpu.make_async_remote_copy(
            src_ref=send_a.at[c, a, pl.ds(kc * rows, rows), :], dst_ref=recv_a.at[slot_chip, slot_core, a],
            send_sem=a_ss.at[c, kc, a], recv_sem=a_rs.at[slot_chip, slot_core, a],
            device_id={"row": c * CORES + kc}, device_id_type=MESH)

    def b_copy(c, kc, slot_chip, slot_core, a):
        return pltpu.make_async_remote_copy(
            src_ref=send_b.at[c, kc, a], dst_ref=recv_b.at[slot_chip, slot_core, a],
            send_sem=b_ss.at[c, kc, a], recv_sem=b_rs.at[slot_chip, slot_core, a],
            device_id={"row": c * CORES + kc}, device_id_type=MESH)

    def near_copy(slot_core, side, a):
        return pltpu.make_async_remote_copy(
            src_ref=near_send.at[side, a], dst_ref=near.at[slot_core, side, a],
            send_sem=near_ss.at[side, a], recv_sem=near_rs.at[side, a],
            device_id={"row": sibling}, device_id_type=MESH)

    combine(0)
    loads[2].wait()
    for c in far_chips:
        for a in range(2):
            send_a[c, a] = to_rows(0, a, c * CORES * rows, CORES * rows)
            for kc in range(CORES):
                a_copy(c, kc, chip, core, a).start()

    make_alpha(1)
    combine(1)
    quarter = rows // 4
    lane_q = lax.broadcasted_iota(jnp.int32, (quarter, wide), 1)
    for c in far_chips:
        for a in range(2):
            result = to_rows(1, a, c * CORES * rows, CORES * rows)
            for kc in range(CORES):
                for k in range(2):
                    piece = result[kc * rows:(kc + 1) * rows, k * wide:(k + 1) * wide]
                    tail = piece[3 * quarter:]
                    for i in range(3):
                        moved = pltpu.roll(tail, wide - drop * (i + 1), 1)
                        send_b[c, kc, a, pl.ds(i * quarter, quarter), pl.ds(k * wide, wide)] = jnp.where(
                            lane_q < drop, moved, piece[i * quarter:(i + 1) * quarter])
                b_copy(c, kc, chip, core, a).start()

    for side in range(2):
        for a in range(2):
            near_send[side, a] = to_rows(side, a, sibling * rows, rows)
            near_copy(core, side, a).start()
    for side in range(2):
        for a in range(2):
            near[core, side, a] = to_rows(side, a, me * rows, rows)

    loads[3].wait()
    chunk = 256
    for side in range(2):
        for a in range(2):
            near_copy(sib_core, side, a).wait_recv()

    def finish(a, side, pieces, write):
        split = [halves(piece) for piece in pieces]
        for x in range(0, 2 * pixels, chunk):
            span = pl.ds(x, chunk)
            value = None
            for k, (hi, lo) in enumerate(split):
                term = dot3(hi, lo, last[0, k, side, :, span], last[1, k, side, :, span])
                value = term if value is None else value + term
            write(a, x, value)

    def write_part(a, x, value):
        part[a, :, pl.ds(x, chunk)] = value

    def write_out(a, x, value):
        value = value + part[a, :, pl.ds(x, chunk)]
        for k in range(chunk // 128):
            woven[x // 128 + k, pl.ds(a, rows, stride=2), :] = value[:, k * 128:(k + 1) * 128]

    for a in range(2):
        pieces = []
        for k in range(CORES):
            value = near[k, 0, a]
            for c in far_chips:
                a_copy(c, k, c, k, a).wait_recv()
                value = value + recv_a[c, k, a]
            pieces.append(value)
        finish(a, 0, pieces, write_part)

    def unpacked(c, k, a):
        sides = []
        for q in range(2):
            lanes = pl.ds(q * wide, wide)
            packed = [recv_b[c, k, a, pl.ds(i * quarter, quarter), lanes] for i in range(3)]
            tail = pltpu.roll(packed[2], 3 * drop, 1)
            for i in (1, 0):
                tail = jnp.where(lane_q < (i + 2) * drop, pltpu.roll(packed[i], (i + 1) * drop, 1), tail)
            sides.append(jnp.concatenate(packed + [tail], axis=0))
        return jnp.concatenate(sides, axis=1)

    for a in range(2):
        pieces = []
        for k in range(CORES):
            value = near[k, 1, a]
            for c in far_chips:
                b_copy(c, k, c, k, a).wait_recv()
                value = value + unpacked(c, k, a)
            pieces.append(value)
        finish(a, 1, pieces, write_out)
    for tile in range(2 * pixels // 128):
        out[:, pl.ds(tile * 128, 128)] = woven[tile]

    for peer in others:
        tot_copy(peer, me).wait_send()
    for g in range(len(groups)):
        send1_copy(core, g).wait_send()
    for a in range(2):
        for side in range(2):
            near_copy(core, side, a).wait_send()
        for c in far_chips:
            for kc in range(CORES):
                a_copy(c, kc, chip, core, a).wait_send()
                b_copy(c, kc, chip, core, a).wait_send()


def solution(mesh):
    count = mesh.shape["row"]

    def per_device(frames, phase_offset, order_gain, band_shift):
        phases, rows, pixels = frames.shape[1:]
        chips = count // CORES
        half = pixels // 2
        wide = half // CORES
        tiles = 4 * (phases // 2) + 2
        lead, column, inverse, last = tables(pixels, count)
        vmem = pl.BlockSpec(memory_space=pltpu.VMEM)
        smem = pl.BlockSpec(memory_space=pltpu.SMEM)
        hbm = pl.BlockSpec(memory_space=pl.ANY)
        bf16, f32 = jnp.bfloat16, jnp.float32
        dma = pltpu.SemaphoreType.DMA
        return pl.pallas_call(
            functools.partial(kernel, count, otf_polynomial()),
            out_shape=pltpu.VMEM((2 * rows, 2 * pixels), f32),
            in_specs=[hbm, smem, smem, smem, hbm, hbm, hbm, hbm],
            out_specs=vmem,
            scratch_shapes=[
                pltpu.VMEM((phases, rows, pixels), bf16),
                pltpu.VMEM(lead.shape, bf16),
                pltpu.VMEM((2, pixels, CORES * rows), bf16),
                pltpu.VMEM(inverse.shape, bf16),
                pltpu.VMEM(last.shape, bf16),
                pltpu.VMEM((8, 128), f32),
                pltpu.VMEM((count, 8, 128), f32),
                pltpu.VMEM((2, phases * rows, pixels), bf16),
                pltpu.VMEM((rows, tiles * wide), f32),
                pltpu.VMEM((CORES * rows, tiles * wide), f32),
                pltpu.VMEM((pixels, tiles * wide), f32),
                pltpu.VMEM((2, 4, phases, half, wide), f32),
                pltpu.VMEM((2, 2, 2, pixels, 2 * wide), bf16),
                pltpu.VMEM((2, 2, rows, 2 * wide), f32),
                pltpu.VMEM((CORES, 2, 2, rows, 2 * wide), f32),
                pltpu.VMEM((chips, 2, CORES * rows, 2 * wide), f32),
                pltpu.VMEM((chips, CORES, 2, rows, 2 * wide), f32),
                pltpu.VMEM((chips, CORES, 2, 3 * rows // 4, 2 * wide), f32),
                pltpu.VMEM((chips, CORES, 2, 3 * rows // 4, 2 * wide), f32),
                pltpu.VMEM((2, rows, 2 * pixels), f32),
                pltpu.VMEM((2 * pixels // 128, 2 * rows, 128), f32),
                dma((phases,)), dma((4,)),
                dma((count,)), dma((count,)),
                dma((phases // 2 + 1,)), dma((phases // 2 + 1,)),
                dma((2, 2)), dma((2, 2)),
                dma((chips, CORES, 2)), dma((chips, CORES, 2)),
                dma((chips, CORES, 2)), dma((chips, CORES, 2)),
            ],
            compiler_params=pltpu.CompilerParams(
                collective_id=0, has_side_effects=True, vmem_limit_bytes=60000000
            ),
        )(frames, phase_offset, order_gain, band_shift,
          jnp.asarray(lead), jnp.asarray(column), jnp.asarray(inverse), jnp.asarray(last))

    in_specs = (P("fov", None, "row", None), P("fov"), P("fov", None), P("fov", None))
    return jax.shard_map(
        per_device, mesh=mesh, in_specs=in_specs, out_specs=P(("fov", "row"), None), check_vma=False
    )
```

```python
import functools
import math

import jax
import jax.numpy as jnp
import numpy as np
from jax import lax
from jax.experimental import pallas as pl
from jax.experimental.pallas import tpu as pltpu
from jax.sharding import PartitionSpec as P

MESH = pl.DeviceIdType.MESH
wiener = 0.1
gain_out = 8.0
cut_share = 0.45
CORES = 2
STEP = 16


def max_shift(pixels):
    return 3 * pixels // 16


def split_table(table):
    high = table.astype(np.float32).astype(jnp.bfloat16)
    low = (table - high.astype(np.float64)).astype(np.float32).astype(jnp.bfloat16)
    return np.stack([high, low])


def cos_sin(points, freqs, length):
    angle = 2.0 * math.pi * ((points[:, None] * freqs[None, :]) % length) / length
    return np.cos(angle), np.sin(angle)


def lane_order(wide):
    drop = wide // 4
    return np.concatenate([np.arange(1, drop + 1), [0], np.arange(drop + 1, wide)])


def tables(pixels, count):
    half = pixels // 2
    wide = half // CORES
    chips = count // CORES
    drop = wide // 4
    points = np.arange(pixels)
    freqs = np.arange(half)
    alternate = 1.0 - 2.0 * (points % 2)
    cos_f, sin_f = cos_sin(points, freqs, pixels)
    sin_f[:, 0] = alternate
    parities = [np.arange(q, half, 2) for q in range(2)]
    order = np.concatenate(parities)
    column = np.concatenate([cos_f[:, order], sin_f[:, order]], axis=1).T
    column = column.reshape(pixels, chips, pixels // chips).transpose(1, 0, 2)
    inverse = []
    for odd in range(2):
        cos_i, sin_i = cos_sin(2 * points[:half] + odd, freqs, 2 * pixels)
        sin_i[:, 0] = alternate[:half]
        inverse.append(np.stack([np.concatenate([cos_i[:, q], sin_i[:, q]], axis=1) for q in parities]))
    inverse = np.stack(inverse)
    lead, last = [], []
    places = np.arange(pixels)
    for core in range(CORES):
        own = CORES * lane_order(wide) + core
        lead.append(np.concatenate([cos_f[:half, own], sin_f[:half, own]], axis=1))
        near_cos, near_sin = cos_sin(places, own, 2 * pixels)
        share = np.where(own == 0, 1.0, 2.0)
        near = np.concatenate([(near_cos * share).T, (-near_sin * share).T])
        mirror = np.where(own == 0, half, pixels - own)
        assert (pixels - own[:drop]).min() > cut_share * pixels + 2 * max_shift(pixels)
        far_cos, far_sin = cos_sin(places, mirror, 2 * pixels)
        keep = np.where(np.arange(wide) < drop, 0.0, 2.0)
        far = np.concatenate([(far_cos * keep).T, (-far_sin * keep).T])
        last.append(np.stack([near, far]))
    return tuple(split_table(t) for t in (np.stack(lead), column, inverse, np.stack(last)))


def otf_polynomial():
    nodes = 0.5 + 0.5 * np.cos(math.pi * (np.arange(64) + 0.5) / 64)
    nodes = np.minimum(nodes, 0.9985)
    root = np.sqrt(1 - nodes * nodes)
    values = 2 / math.pi * (np.arccos(nodes) - nodes * root) / root**3
    fit = np.polynomial.chebyshev.Chebyshev.fit(nodes, values, 9, domain=[0, 1])
    poly = fit.convert(kind=np.polynomial.Polynomial).coef
    return [float(c) for c in poly[::-1]]


def halves(value):
    high = value.astype(jnp.bfloat16)
    return high, (value - high.astype(jnp.float32)).astype(jnp.bfloat16)


def dot(left, right):
    return jnp.dot(left, right, preferred_element_type=jnp.float32)


def dot3(left_hi, left_lo, right_hi, right_lo):
    return dot(left_hi, right_hi) + (dot(left_hi, right_lo) + dot(left_lo, right_hi))


def kernel(count, poly, frames_h, offset, gain, shift, lead_h, column_h, inverse_h, last_h, out,
           frames, lead, column, inverse, last, tot_send, tot, folds, ramps, planes, spec, mixed, alpha, coef,
           near_send, near, send_a, recv_a, send_b, recv_b, part, woven,
           frame_sem, table_sem, tot_ss, tot_rs, fold_ss, fold_rs, near_ss, near_rs, a_ss, a_rs, b_ss, b_rs):
    me = lax.axis_index("row")
    chips = count // CORES
    chip, core = me // CORES, me % CORES
    sib_core = 1 - core
    phases, rows, pixels = frames.shape
    half = pixels // 2
    wide = half // CORES
    drop = wide // 4
    orders = phases // 2
    mid = phases // 2
    others = [lax.rem(me + step, count) for step in range(1, count)]
    far_chips = [lax.rem(chip + step, chips) for step in range(1, chips)]
    sibling = chip * CORES + sib_core

    barrier = pltpu.get_barrier_semaphore()
    for peer in others:
        pl.semaphore_signal(barrier, inc=1, device_id={"row": peer}, device_id_type=MESH)
    frame_loads = []
    for p in range(phases):
        frame_loads.append(pltpu.make_async_copy(frames_h.at[0, p], frames.at[p], frame_sem.at[p]))
        frame_loads[p].start()
    loads = []
    for idx, (source, target) in enumerate(
        ((lead_h.at[:, core], lead), (column_h.at[:, chip], column), (inverse_h, inverse), (last_h, last))
    ):
        loads.append(pltpu.make_async_copy(source, target, table_sem.at[idx]))
    loads[0].start()

    mine = pl.ds(pl.multiple_of(core * rows, rows), rows)
    lane8 = lax.broadcasted_iota(jnp.int32, (8, 128), 1)
    total_part = jnp.zeros((8, 128), jnp.float32)
    for p in range(phases):
        frame_loads[p].wait()
        lower, upper = frames[p, :, :half].astype(jnp.float32), frames[p, :, half:].astype(jnp.float32)
        both = lower + upper
        folds[0, p, mine, :] = both
        folds[1, p, mine, :] = lower - upper
        s = jnp.sum(jnp.sum(both, axis=0, keepdims=True), axis=1, keepdims=True)
        total_part = total_part + jnp.where(lane8 == p, s, 0.0)
    tot_send[...] = total_part
    tot[me] = total_part
    pl.semaphore_wait(barrier, count - 1)

    def tot_copy(peer, slot):
        return pltpu.make_async_remote_copy(
            src_ref=tot_send, dst_ref=tot.at[slot], send_sem=tot_ss.at[peer], recv_sem=tot_rs.at[slot],
            device_id={"row": peer}, device_id_type=MESH)

    for peer in others:
        tot_copy(peer, me).start()

    def fold_copy(slot_core, k):
        place = pl.ds(pl.multiple_of(slot_core * rows, rows), rows)
        return pltpu.make_async_remote_copy(
            src_ref=folds.at[k, :, place], dst_ref=folds.at[k, :, place],
            send_sem=fold_ss.at[k], recv_sem=fold_rs.at[k],
            device_id={"row": sibling}, device_id_type=MESH)

    for k in range(2):
        fold_copy(core, k).start()
    for load in loads[1:]:
        load.start()

    shift_y, shift_x = shift[0, 0], shift[0, 1]
    inv_cut = 1.0 / (cut_share * pixels)
    scale_out = 0.5 * gain_out / (4.0 * pixels * pixels)
    gains = [gain[0, j] for j in range(phases)]
    squares = [g * g for g in gains]
    scaled = [g * scale_out for g in gains]
    reach = int(cut_share * pixels) + 1 + 2 * max_shift(pixels)
    single = max((pixels - reach) // 2 // STEP, 1)
    quarter = half // 2

    def blocks(block, few, many):
        for odd in range(2):
            def body(which, i, carry):
                block(pl.multiple_of(i * STEP, STEP), odd, which, False)
                return carry

            lax.fori_loop(1 - odd, single, functools.partial(body, few), 0)
            lax.fori_loop(single, quarter // STEP, functools.partial(body, many), 0)

    def own_freq(shape):
        lane = lax.broadcasted_iota(jnp.int32, shape, 1)
        place = jnp.where(lane < drop, lane + 1, jnp.where(lane == drop, 0, lane))
        return CORES * place + core

    def make_alpha(side):
        freq = own_freq((STEP, wide))
        if side:
            freq = jnp.where(freq == 0, half, pixels - freq)
        used = [j for j in range(phases) if not (side and j == mid)]
        sq_xs = {}
        for j in used:
            fx = (freq - (j - mid) * shift_x).astype(jnp.float32) * inv_cut
            sq_xs[j] = fx * fx + 1e-30
        offs = {j: ((j - mid) * shift_y).astype(jnp.float32) * inv_cut for j in used}

        def block(first, odd, slots, top):
            row = 2 * (first + lax.broadcasted_iota(jnp.int32, (STEP, wide), 0)) + odd
            here = pl.ds(odd * quarter + first, STEP)
            for slot in slots:
                big_y = row if slot % 2 == 0 else -row
                if top and slot % 2:
                    big_y = jnp.where(row == 0, -half, big_y)
                if slot == 2:
                    big_y = big_y - pixels
                if slot == 3:
                    big_y = big_y + pixels
                unit_y = big_y.astype(jnp.float32) * inv_cut
                den = jnp.full((STEP, wide), wiener, jnp.float32)
                den_m = jnp.full((STEP, wide), wiener, jnp.float32)
                values = {}
                for j in used:
                    fy = unit_y - offs[j]
                    t = fy * fy + sq_xs[j]
                    r = t * lax.rsqrt(t)
                    u = jnp.maximum(1.0 - t, 1e-30)
                    v = u * lax.rsqrt(u)
                    acc = poly[0] * r + poly[1]
                    for c in poly[2:]:
                        acc = acc * r + c
                    value = acc * (u * v)
                    values[j] = value
                    sq = value * value
                    den = den + squares[j] * sq
                    den_m = den_m + squares[phases - 1 - j] * sq
                both = 1.0 / (den * den_m)
                inv, inv_m = den_m * both, den * both
                for j in used:
                    alpha[side, slot, j, here, :] = values[j] * (
                        scaled[j] * inv + scaled[phases - 1 - j] * inv_m)

        block(0, 0, (0, 1, 2, 3), True)
        blocks(block, (0, 1), (0, 1, 2, 3))

    turn = 2.0 * math.pi / pixels

    def ramp(points, step):
        arg = ((points * step) & (pixels - 1)).astype(jnp.float32) * turn
        return jnp.cos(arg), jnp.sin(arg)

    def times(left, right):
        return left[0] * right[0] - left[1] * right[1], left[0] * right[1] + left[1] * right[0]

    row8 = lax.broadcasted_iota(jnp.int32, (8, 128), 0) + chip * (CORES * rows)
    wave_x = [ramp(lane8 + 128 * k, shift_x) for k in range(half // 128)]
    base = ramp(row8, shift_y)
    leap = ramp(jnp.full((8, 128), 8, jnp.int32), shift_y)
    pieces = [base]
    for k in range(1, CORES * rows // 8):
        pieces.append(times(pieces[-1], leap))
    wave_y = tuple(jnp.concatenate([q[k] for q in pieces], axis=0) for k in range(2))
    start = jnp.full((8, 128), offset[0], jnp.float32)
    wave_x = [times(w, (jnp.cos(start), -jnp.sin(start))) for w in wave_x]
    for k in range(half // 128):
        turned = times(wave_y, (wave_x[k][0][:1], wave_x[k][1][:1]))
        value = turned
        for order in range(orders):
            if order:
                value = times(value, turned)
            for q in range(2):
                ramps[order, q, :, pl.ds(k * 128, 128)] = value[q]

    make_alpha(0)

    for peer in others:
        tot_copy(peer, peer).wait_recv()
    total = tot[0]
    for d in range(1, count):
        total = total + tot[d]
    level = jnp.where(lane8 < phases, float(pixels * pixels), 0.0) / jnp.where(lane8 < phases, total, 1.0)
    level = level / phases

    groups = [(4 * g, 4, g + 1) for g in range(orders)] + [(4 * orders, 2, 0)]

    span_rows = CORES * rows

    def scaled_folds(which, rows_at, lanes_at):
        return [level[:1, p:p + 1] * folds[which, p, rows_at, lanes_at] for p in range(phases)]

    def modulated(order, values, rows_at, lanes_at):
        re, im = values[0], None
        for q in range(1, mid + 1):
            theta = 2.0 * math.pi * order * q / phases
            re = re + math.cos(theta) * (values[q] + values[phases - q])
            term = -math.sin(theta) * (values[q] - values[phases - q])
            im = term if im is None else im + term
        return times((re, im), [ramps[order - 1, k, rows_at, lanes_at] for k in range(2)])

    swapped = core + (shift_x & 1) * (1 - 2 * core)

    def unmix(wanted):
        which = swapped if wanted[0] % 2 else core
        for r in range(0, span_rows, STEP):
            for x in range(0, half, 128):
                rows_at, lanes_at = pl.ds(r, STEP), pl.ds(x, 128)
                values = scaled_folds(which, rows_at, lanes_at)
                for order in wanted:
                    if order:
                        made = modulated(order, values, rows_at, lanes_at)
                    else:
                        made = [functools.reduce(lambda a, b: a + b, values)]
                    for k, value in enumerate(made):
                        hi, lo = halves(value)
                        place = (2 * (order - 1) if order else 2 * orders) + k
                        planes[0, pl.ds(place * span_rows + r, STEP), lanes_at] = hi
                        planes[1, pl.ds(place * span_rows + r, STEP), lanes_at] = lo

    def spectrum(g):
        first, tiles, order = groups[g]
        place = 2 * (order - 1) if order else 2 * orders
        span = pl.ds(place * span_rows, (2 if order else 1) * span_rows)
        result = dot3(planes[0, span, :], planes[1, span, :], lead[0], lead[1])
        special = jnp.logical_and(
            lax.broadcasted_iota(jnp.int32, (span_rows, wide), 1) == drop, core == 0)
        if order:
            cr, sr = result[:span_rows, :wide], result[:span_rows, wide:]
            ci, si = result[span_rows:, :wide], result[span_rows:, wide:]
            values = [jnp.where(special, cr, cr + si), jnp.where(special, ci, ci - sr),
                      jnp.where(special, sr, cr - si), jnp.where(special, si, ci + sr)]
        else:
            values = [result[:, :wide], jnp.where(special, 0.0, -result[:, wide:])]
        for k, value in enumerate(values):
            hi, lo = halves(value)
            spec[0, :, pl.ds((first + k) * wide, wide)] = hi
            spec[1, :, pl.ds((first + k) * wide, wide)] = lo
        window = pl.ds(first * wide, tiles * wide)
        mixed[:, window] = dot3(column[0], column[1], spec[0, :, window], spec[1, :, window])

    for load in loads[:2]:
        load.wait()
    for k in range(2):
        fold_copy(sib_core, k).wait_recv()
    for order in range(1, orders + 1, 2):
        unmix([order])
        spectrum(order - 1)
    unmix(list(range(2, orders + 1, 2)) + [0])
    for order in range(2, orders + 1, 2):
        spectrum(order - 1)
    spectrum(orders)

    special = jnp.logical_and(lax.broadcasted_iota(jnp.int32, (STEP, wide), 1) == drop, core == 0)

    def combine(side):
        def block(first, odd, second, top):
            here, below = pl.ds(odd * quarter + first, STEP), pl.ds(half + odd * quarter + first, STEP)
            upper, lower = pl.ds(first, STEP), pl.ds(quarter + first, STEP)
            row0 = None
            if top:
                row0 = lax.broadcasted_iota(jnp.int32, (STEP, wide), 0) == 0

            def pick(at_top, value):
                return jnp.where(row0, at_top, value) if top else value

            def signs(tile):
                re, im = pl.ds(tile * wide, wide), pl.ds((tile + 1) * wide, wide)
                cr, ci, sr, si = mixed[here, re], mixed[here, im], mixed[below, re], mixed[below, im]
                plus = (pick(cr, cr + si), pick(ci, ci - sr))
                minus = (pick(sr, cr - si), pick(si, ci + sr))
                return plus, minus

            slots = (0, 1, 2, 3) if second else (0, 1)
            sums = {slot: [None, None] for slot in slots}

            def add(slot, k, term):
                sums[slot][k] = term if sums[slot][k] is None else sums[slot][k] + term

            if side == 0:
                center = signs(4 * orders)
                for slot in slots:
                    a = alpha[side, slot, mid, here, :]
                    for k in range(2):
                        add(slot, k, a * center[slot % 2][k])
            for order in range(1, orders + 1):
                pos, neg = signs(4 * (order - 1)), signs(4 * (order - 1) + 2)
                direct, other = (pos, neg) if side == 0 else (neg, pos)
                partner = [[jnp.where(special, direct[s][k], other[s][k]) for k in range(2)] for s in range(2)]
                if top:
                    swap = [[pick(partner[s][k], partner[1 - s][k]) for k in range(2)] for s in range(2)]
                else:
                    swap = [partner[1], partner[0]]
                for slot in slots:
                    s = slot % 2
                    up, down = alpha[side, slot, mid + order, here, :], alpha[side, slot, mid - order, here, :]
                    add(slot, 0, up * direct[s][0] + down * swap[s][0])
                    add(slot, 1, up * direct[s][1] - down * swap[s][1])
            for a in range(2):
                def folded(s, k):
                    if not second:
                        return sums[s][k]
                    return sums[s][k] + sums[2 + s][k] if a == 0 else sums[s][k] - sums[2 + s][k]

                pr, pi, mr, mi = folded(0, 0), folded(0, 1), folded(1, 0), folded(1, 1)
                low_top = (mr, mi) if a == 0 else (mi, -mr)
                values = [(upper, 0, pick(pr, pr + mr)), (upper, 1, pick(pi, pi + mi)),
                          (lower, 0, pick(low_top[0], mi - pi)), (lower, 1, pick(low_top[1], pr - mr))]
                for place, k, value in values:
                    hi, lo = halves(value)
                    coef[0, side, a, odd, place, pl.ds(k * wide, wide)] = hi
                    coef[1, side, a, odd, place, pl.ds(k * wide, wide)] = lo

        block(0, 0, True, True)
        blocks(block, False, True)

    flip = jnp.where(chip == 0, 1.0, -1.0)

    def to_rows(side, a):
        even, odd = [dot3(inverse[0, a, q], inverse[1, a, q], coef[0, side, a, q], coef[1, side, a, q])
                     for q in range(2)]
        odd = odd * flip
        return even + odd, even - odd

    def keep_near(side, a, value):
        first, second = value[:rows], value[rows:]
        near[core, side, a] = jnp.where(core == 0, first, second)
        near_send[side, a] = jnp.where(core == 0, second, first)
        near_copy(core, side, a).start()

    def a_copy(c, kc, slot_chip, slot_core, a):
        return pltpu.make_async_remote_copy(
            src_ref=send_a.at[c, a, pl.ds(kc * rows, rows), :], dst_ref=recv_a.at[slot_chip, slot_core, a],
            send_sem=a_ss.at[c, kc, a], recv_sem=a_rs.at[slot_chip, slot_core, a],
            device_id={"row": c * CORES + kc}, device_id_type=MESH)

    def b_copy(c, kc, slot_chip, slot_core, a):
        return pltpu.make_async_remote_copy(
            src_ref=send_b.at[c, kc, a], dst_ref=recv_b.at[slot_chip, slot_core, a],
            send_sem=b_ss.at[c, kc, a], recv_sem=b_rs.at[slot_chip, slot_core, a],
            device_id={"row": c * CORES + kc}, device_id_type=MESH)

    def near_copy(slot_core, side, a):
        return pltpu.make_async_remote_copy(
            src_ref=near_send.at[side, a], dst_ref=near.at[slot_core, side, a],
            send_sem=near_ss.at[side, a], recv_sem=near_rs.at[side, a],
            device_id={"row": sibling}, device_id_type=MESH)

    combine(0)
    loads[2].wait()
    for c in far_chips:
        for a in range(2):
            own_rows, far_rows = to_rows(0, a)
            send_a[c, a] = far_rows
            for kc in range(CORES):
                a_copy(c, kc, chip, core, a).start()
            keep_near(0, a, own_rows)

    make_alpha(1)
    combine(1)
    fourth = rows // 4
    lane_q = lax.broadcasted_iota(jnp.int32, (fourth, wide), 1)
    for c in far_chips:
        for a in range(2):
            own_rows, far_rows = to_rows(1, a)
            for kc in range(CORES):
                for k in range(2):
                    piece = far_rows[kc * rows:(kc + 1) * rows, k * wide:(k + 1) * wide]
                    tail = piece[3 * fourth:]
                    for i in range(3):
                        moved = pltpu.roll(tail, wide - drop * (i + 1), 1)
                        send_b[c, kc, a, pl.ds(i * fourth, fourth), pl.ds(k * wide, wide)] = jnp.where(
                            lane_q < drop, moved, piece[i * fourth:(i + 1) * fourth])
                b_copy(c, kc, chip, core, a).start()
            keep_near(1, a, own_rows)

    loads[3].wait()
    chunk = 256
    for side in range(2):
        for a in range(2):
            near_copy(sib_core, side, a).wait_recv()

    def finish(a, side, pieces, write):
        split = [halves(piece) for piece in pieces]
        for x in range(0, pixels, chunk):
            span = pl.ds(x, chunk)
            even, odd = [dot3(hi, lo, last[0, k, side, :, span], last[1, k, side, :, span])
                         for k, (hi, lo) in enumerate(split)]
            write(a, x, even + odd)
            write(a, pixels + x, even - odd)

    def write_part(a, x, value):
        part[a, :, pl.ds(x, chunk)] = value

    def write_out(a, x, value):
        value = value + part[a, :, pl.ds(x, chunk)]
        for k in range(chunk // 128):
            woven[x // 128 + k, pl.ds(a, rows, stride=2), :] = value[:, k * 128:(k + 1) * 128]

    for a in range(2):
        pieces = []
        for k in range(CORES):
            value = near[k, 0, a]
            for c in far_chips:
                a_copy(c, k, c, k, a).wait_recv()
                value = value + recv_a[c, k, a]
            pieces.append(value)
        finish(a, 0, pieces, write_part)

    def unpacked(c, k, a):
        sides = []
        for q in range(2):
            lanes = pl.ds(q * wide, wide)
            packed = [recv_b[c, k, a, pl.ds(i * fourth, fourth), lanes] for i in range(3)]
            tail = pltpu.roll(packed[2], 3 * drop, 1)
            for i in (1, 0):
                tail = jnp.where(lane_q < (i + 2) * drop, pltpu.roll(packed[i], (i + 1) * drop, 1), tail)
            sides.append(jnp.concatenate(packed + [tail], axis=0))
        return jnp.concatenate(sides, axis=1)

    for a in range(2):
        pieces = []
        for k in range(CORES):
            value = near[k, 1, a]
            for c in far_chips:
                b_copy(c, k, c, k, a).wait_recv()
                value = value + unpacked(c, k, a)
            pieces.append(value)
        finish(a, 1, pieces, write_out)
    for tile in range(2 * pixels // 128):
        out[:, pl.ds(tile * 128, 128)] = woven[tile]

    for peer in others:
        tot_copy(peer, me).wait_send()
    for k in range(2):
        fold_copy(core, k).wait_send()
    for a in range(2):
        for side in range(2):
            near_copy(core, side, a).wait_send()
        for c in far_chips:
            for kc in range(CORES):
                a_copy(c, kc, chip, core, a).wait_send()
                b_copy(c, kc, chip, core, a).wait_send()


def solution(mesh):
    count = mesh.shape["row"]

    def per_device(frames, phase_offset, order_gain, band_shift):
        phases, rows, pixels = frames.shape[1:]
        chips = count // CORES
        assert chips == 2 and CORES == 2
        half = pixels // 2
        wide = half // CORES
        tiles = 4 * (phases // 2) + 2
        lead, column, inverse, last = tables(pixels, count)
        vmem = pl.BlockSpec(memory_space=pltpu.VMEM)
        smem = pl.BlockSpec(memory_space=pltpu.SMEM)
        hbm = pl.BlockSpec(memory_space=pl.ANY)
        bf16, f32 = jnp.bfloat16, jnp.float32
        dma = pltpu.SemaphoreType.DMA
        return pl.pallas_call(
            functools.partial(kernel, count, otf_polynomial()),
            out_shape=pltpu.VMEM((2 * rows, 2 * pixels), f32),
            in_specs=[hbm, smem, smem, smem, hbm, hbm, hbm, hbm],
            out_specs=vmem,
            scratch_shapes=[
                pltpu.VMEM((phases, rows, pixels), bf16),
                pltpu.VMEM((2, half, 2 * wide), bf16),
                pltpu.VMEM((2, pixels, CORES * rows), bf16),
                pltpu.VMEM(inverse.shape, bf16),
                pltpu.VMEM(last.shape, bf16),
                pltpu.VMEM((8, 128), f32),
                pltpu.VMEM((count, 8, 128), f32),
                pltpu.VMEM((2, phases, CORES * rows, half), f32),
                pltpu.VMEM((phases // 2, 2, CORES * rows, half), f32),
                pltpu.VMEM((2, phases * CORES * rows, half), bf16),
                pltpu.VMEM((2, CORES * rows, tiles * wide), bf16),
                pltpu.VMEM((pixels, tiles * wide), f32),
                pltpu.VMEM((2, 4, phases, half, wide), f32),
                pltpu.VMEM((2, 2, 2, 2, half, 2 * wide), bf16),
                pltpu.VMEM((2, 2, rows, 2 * wide), f32),
                pltpu.VMEM((CORES, 2, 2, rows, 2 * wide), f32),
                pltpu.VMEM((chips, 2, CORES * rows, 2 * wide), f32),
                pltpu.VMEM((chips, CORES, 2, rows, 2 * wide), f32),
                pltpu.VMEM((chips, CORES, 2, 3 * rows // 4, 2 * wide), f32),
                pltpu.VMEM((chips, CORES, 2, 3 * rows // 4, 2 * wide), f32),
                pltpu.VMEM((2, rows, 2 * pixels), f32),
                pltpu.VMEM((2 * pixels // 128, 2 * rows, 128), f32),
                dma((phases,)), dma((4,)),
                dma((count,)), dma((count,)),
                dma((2,)), dma((2,)),
                dma((2, 2)), dma((2, 2)),
                dma((chips, CORES, 2)), dma((chips, CORES, 2)),
                dma((chips, CORES, 2)), dma((chips, CORES, 2)),
            ],
            compiler_params=pltpu.CompilerParams(
                collective_id=0, has_side_effects=True, vmem_limit_bytes=60000000
            ),
        )(frames, phase_offset, order_gain, band_shift,
          jnp.asarray(lead), jnp.asarray(column), jnp.asarray(inverse), jnp.asarray(last))

    in_specs = (P("fov", None, "row", None), P("fov"), P("fov", None), P("fov", None))
    return jax.shard_map(
        per_device, mesh=mesh, in_specs=in_specs, out_specs=P(("fov", "row"), None), check_vma=False
    )
```

```python
import functools
import math

import jax
import jax.numpy as jnp
import numpy as np
from jax import lax
from jax.experimental import pallas as pl
from jax.experimental.pallas import tpu as pltpu
from jax.sharding import PartitionSpec as P

MESH = pl.DeviceIdType.MESH
wiener = 0.1
gain_out = 8.0
cut_share = 0.45
CORES = 2
STEP = 16


def max_shift(pixels):
    return 3 * pixels // 16


def split_table(table):
    high = table.astype(np.float32).astype(jnp.bfloat16)
    low = (table - high.astype(np.float64)).astype(np.float32).astype(jnp.bfloat16)
    return np.stack([high, low])


def cos_sin(points, freqs, length):
    angle = 2.0 * math.pi * ((points[:, None] * freqs[None, :]) % length) / length
    return np.cos(angle), np.sin(angle)


def lane_order(wide):
    drop = (wide + 1) // 3
    return np.concatenate([np.arange(1, drop + 1), [0], np.arange(drop + 1, wide)])


def tables(pixels, count):
    half = pixels // 2
    wide = half // CORES
    chips = count // CORES
    drop = (wide + 1) // 3
    points = np.arange(pixels)
    freqs = np.arange(half)
    alternate = 1.0 - 2.0 * (points % 2)
    cos_f, sin_f = cos_sin(points, freqs, pixels)
    sin_f[:, 0] = alternate
    parities = [np.arange(q, half, 2) for q in range(2)]
    order = np.concatenate(parities)
    column = np.concatenate([cos_f[:, order], sin_f[:, order]], axis=1).T
    column = column.reshape(pixels, chips, pixels // chips).transpose(1, 0, 2)
    inverse = []
    for odd in range(2):
        cos_i, sin_i = cos_sin(2 * points[:half] + odd, freqs, 2 * pixels)
        sin_i[:, 0] = alternate[:half]
        inverse.append(np.stack([np.concatenate([cos_i[:, q], sin_i[:, q]], axis=1) for q in parities]))
    inverse = np.stack(inverse)
    lead, last = [], []
    places = np.arange(pixels)
    for core in range(CORES):
        own = CORES * lane_order(wide) + core
        lead.append(np.concatenate([cos_f[:half, own], sin_f[:half, own]], axis=1))
        near_cos, near_sin = cos_sin(places, own, 2 * pixels)
        share = np.where(own == 0, 1.0, 2.0)
        near = np.concatenate([(near_cos * share).T, (-near_sin * share).T])
        mirror = np.where(own == 0, half, pixels - own)
        assert (pixels - own[:drop]).min() > cut_share * pixels + 2 * max_shift(pixels)
        far_cos, far_sin = cos_sin(places, mirror, 2 * pixels)
        keep = np.where(np.arange(wide) < drop, 0.0, 2.0)
        far = np.concatenate([(far_cos * keep).T, (-far_sin * keep).T])
        last.append(np.stack([near, far]))
    return tuple(split_table(t) for t in (np.stack(lead), column, inverse, np.stack(last)))


def otf_polynomial():
    nodes = 0.5 + 0.5 * np.cos(math.pi * (np.arange(64) + 0.5) / 64)
    nodes = np.minimum(nodes, 0.9985)
    values = 2 / math.pi * (np.arccos(nodes) - nodes * np.sqrt(1 - nodes * nodes)) / (1 - nodes) ** 1.5
    fit = np.polynomial.chebyshev.Chebyshev.fit(nodes, values, 6, domain=[0, 1])
    poly = fit.convert(kind=np.polynomial.Polynomial).coef
    return [float(c) for c in poly[::-1]]


def halves(value):
    high = value.astype(jnp.bfloat16)
    return high, (value - high.astype(jnp.float32)).astype(jnp.bfloat16)


def dot(left, right):
    return jnp.dot(left, right, preferred_element_type=jnp.float32)


def dot3(left_hi, left_lo, right_hi, right_lo):
    return dot(left_hi, right_hi) + (dot(left_hi, right_lo) + dot(left_lo, right_hi))


def kernel(count, poly, frames_h, offset_h, gain_h, shift_h, lead_h, column_h, inverse_h, last_h, out,
           offset, gain, shift, frames, lead, column, inverse, last, tot_send, tot, folds, ramps, planes, spec, mixed, alpha, coef,
           near_send, near, send_a, recv_a, send_b, recv_b, part, woven,
           small_sem, frame_sem, table_sem, tot_ss, tot_rs, fold_ss, fold_rs, near_ss, near_rs, a_ss, a_rs, b_ss, b_rs):
    me = lax.axis_index("row")
    chips = count // CORES
    chip, core = me // CORES, me % CORES
    sib_core = 1 - core
    phases, rows, pixels = frames.shape
    half = pixels // 2
    wide = half // CORES
    drop = (wide + 1) // 3
    orders = phases // 2
    mid = phases // 2
    others = [lax.rem(me + step, count) for step in range(1, count)]
    far_chips = [lax.rem(chip + step, chips) for step in range(1, chips)]
    sibling = chip * CORES + sib_core

    barrier = pltpu.get_barrier_semaphore()
    for peer in others:
        pl.semaphore_signal(barrier, inc=1, device_id={"row": peer}, device_id_type=MESH)
    frame_loads = []
    for p in range(phases):
        frame_loads.append(pltpu.make_async_copy(frames_h.at[0, p], frames.at[p], frame_sem.at[p]))
        frame_loads[p].start()
    small = []
    for idx, (source, target) in enumerate(((offset_h, offset), (gain_h, gain), (shift_h, shift))):
        small.append(pltpu.make_async_copy(source, target, small_sem.at[idx]))
        small[idx].start()
    loads = []
    for idx, (source, target) in enumerate(
        ((lead_h.at[:, core], lead), (column_h.at[:, chip], column), (inverse_h, inverse), (last_h, last))
    ):
        loads.append(pltpu.make_async_copy(source, target, table_sem.at[idx]))
    loads[0].start()

    mine = pl.ds(pl.multiple_of(core * rows, rows), rows)
    lane8 = lax.broadcasted_iota(jnp.int32, (8, 128), 1)
    total_part = jnp.zeros((8, 128), jnp.float32)
    for p in range(phases):
        frame_loads[p].wait()
        lower, upper = frames[p, :, :half].astype(jnp.float32), frames[p, :, half:].astype(jnp.float32)
        both = lower + upper
        folds[0, p, mine, :] = both
        folds[1, p, mine, :] = lower - upper
        s = jnp.sum(jnp.sum(both, axis=0, keepdims=True), axis=1, keepdims=True)
        total_part = total_part + jnp.where(lane8 == p, s, 0.0)
    tot_send[...] = total_part
    tot[me] = total_part
    pl.semaphore_wait(barrier, count - 1)

    def tot_copy(peer, slot):
        return pltpu.make_async_remote_copy(
            src_ref=tot_send, dst_ref=tot.at[slot], send_sem=tot_ss.at[peer], recv_sem=tot_rs.at[slot],
            device_id={"row": peer}, device_id_type=MESH)

    for peer in others:
        tot_copy(peer, me).start()

    def fold_copy(slot_core, k):
        place = pl.ds(pl.multiple_of(slot_core * rows, rows), rows)
        return pltpu.make_async_remote_copy(
            src_ref=folds.at[k, :, place], dst_ref=folds.at[k, :, place],
            send_sem=fold_ss.at[k], recv_sem=fold_rs.at[k],
            device_id={"row": sibling}, device_id_type=MESH)

    for k in range(2):
        fold_copy(core, k).start()
    for load in loads[1:]:
        load.start()

    for load in small:
        load.wait()
    shift_y, shift_x = shift[0, 0], shift[0, 1]
    inv_cut = 1.0 / (cut_share * pixels)
    scale_out = 0.5 * gain_out / (4.0 * pixels * pixels)
    gains = [gain[0, j] for j in range(phases)]
    squares = [g * g for g in gains]
    scaled = [g * scale_out for g in gains]
    reach = int(cut_share * pixels) + 1 + 2 * max_shift(pixels)
    single = max((pixels - reach) // 2 // STEP, 1)
    quarter = half // 2

    def blocks(block, few, many):
        for odd in range(2):
            def body(which, i, carry):
                block(pl.multiple_of(i * STEP, STEP), odd, which, False)
                return carry

            lax.fori_loop(1 - odd, single, functools.partial(body, few), 0)
            lax.fori_loop(single, quarter // STEP, functools.partial(body, many), 0)

    def own_freq(shape):
        lane = lax.broadcasted_iota(jnp.int32, shape, 1)
        place = jnp.where(lane < drop, lane + 1, jnp.where(lane == drop, 0, lane))
        return CORES * place + core

    def make_alpha(side):
        freq = own_freq((STEP, wide))
        if side:
            freq = jnp.where(freq == 0, half, pixels - freq)
        used = [j for j in range(phases) if not (side and j == mid)]
        sq_xs = {}
        for j in used:
            fx = (freq - (j - mid) * shift_x).astype(jnp.float32) * inv_cut
            sq_xs[j] = fx * fx + 1e-30
        offs = {j: ((j - mid) * shift_y).astype(jnp.float32) * inv_cut for j in used}

        def block(first, odd, slots, top):
            row = 2 * (first + lax.broadcasted_iota(jnp.int32, (STEP, wide), 0)) + odd
            here = pl.ds(odd * quarter + first, STEP)
            for slot in slots:
                big_y = row if slot % 2 == 0 else -row
                if top and slot % 2:
                    big_y = jnp.where(row == 0, -half, big_y)
                if slot == 2:
                    big_y = big_y - pixels
                if slot == 3:
                    big_y = big_y + pixels
                unit_y = big_y.astype(jnp.float32) * inv_cut
                den = jnp.full((STEP, wide), wiener, jnp.float32)
                den_m = jnp.full((STEP, wide), wiener, jnp.float32)
                values = {}
                for j in used:
                    fy = unit_y - offs[j]
                    t = fy * fy + sq_xs[j]
                    r = t * lax.rsqrt(t)
                    u = jnp.maximum(1.0 - r, 1e-30)
                    v = u * lax.rsqrt(u)
                    acc = poly[0] * r + poly[1]
                    for c in poly[2:]:
                        acc = acc * r + c
                    value = acc * (u * v)
                    values[j] = value
                    sq = value * value
                    den = den + squares[j] * sq
                    den_m = den_m + squares[phases - 1 - j] * sq
                both = 1.0 / (den * den_m)
                inv, inv_m = den_m * both, den * both
                for j in used:
                    alpha[side, slot, j, here, :] = values[j] * (
                        scaled[j] * inv + scaled[phases - 1 - j] * inv_m)

        block(0, 0, (0, 1, 2, 3), True)
        blocks(block, (0, 1), (0, 1, 2, 3))

    turn = 2.0 * math.pi / pixels

    def ramp(points, step):
        arg = ((points * step) & (pixels - 1)).astype(jnp.float32) * turn
        return jnp.cos(arg), jnp.sin(arg)

    def times(left, right):
        return left[0] * right[0] - left[1] * right[1], left[0] * right[1] + left[1] * right[0]

    row8 = lax.broadcasted_iota(jnp.int32, (8, 128), 0) + chip * (CORES * rows)
    wave_x = [ramp(lane8 + 128 * k, shift_x) for k in range(half // 128)]
    base = ramp(row8, shift_y)
    leap = ramp(jnp.full((8, 128), 8, jnp.int32), shift_y)
    pieces = [base]
    for k in range(1, CORES * rows // 8):
        pieces.append(times(pieces[-1], leap))
    wave_y = tuple(jnp.concatenate([q[k] for q in pieces], axis=0) for k in range(2))
    start = jnp.full((8, 128), offset[0], jnp.float32)
    wave_x = [times(w, (jnp.cos(start), -jnp.sin(start))) for w in wave_x]
    for k in range(half // 128):
        turned = times(wave_y, (wave_x[k][0][:1], wave_x[k][1][:1]))
        value = turned
        for order in range(orders):
            if order:
                value = times(value, turned)
            for q in range(2):
                ramps[order, q, :, pl.ds(k * 128, 128)] = value[q]

    make_alpha(0)

    for peer in others:
        tot_copy(peer, peer).wait_recv()
    total = tot[0]
    for d in range(1, count):
        total = total + tot[d]
    level = jnp.where(lane8 < phases, float(pixels * pixels), 0.0) / jnp.where(lane8 < phases, total, 1.0)
    level = level / phases

    groups = [(4 * g, 4, g + 1) for g in range(orders)] + [(4 * orders, 2, 0)]

    span_rows = CORES * rows

    def scaled_folds(which, rows_at, lanes_at):
        return [level[:1, p:p + 1] * folds[which, p, rows_at, lanes_at] for p in range(phases)]

    def modulated(order, values, rows_at, lanes_at):
        re, im = values[0], None
        for q in range(1, mid + 1):
            theta = 2.0 * math.pi * order * q / phases
            re = re + math.cos(theta) * (values[q] + values[phases - q])
            term = -math.sin(theta) * (values[q] - values[phases - q])
            im = term if im is None else im + term
        return times((re, im), [ramps[order - 1, k, rows_at, lanes_at] for k in range(2)])

    swapped = core + (shift_x & 1) * (1 - 2 * core)

    def unmix(wanted):
        which = swapped if wanted[0] % 2 else core
        for r in range(0, span_rows, STEP):
            for x in range(0, half, 128):
                rows_at, lanes_at = pl.ds(r, STEP), pl.ds(x, 128)
                values = scaled_folds(which, rows_at, lanes_at)
                for order in wanted:
                    if order:
                        made = modulated(order, values, rows_at, lanes_at)
                    else:
                        made = [functools.reduce(lambda a, b: a + b, values)]
                    for k, value in enumerate(made):
                        hi, lo = halves(value)
                        place = (2 * (order - 1) if order else 2 * orders) + k
                        planes[0, pl.ds(place * span_rows + r, STEP), lanes_at] = hi
                        planes[1, pl.ds(place * span_rows + r, STEP), lanes_at] = lo

    def spectrum(g):
        first, tiles, order = groups[g]
        place = 2 * (order - 1) if order else 2 * orders
        span = pl.ds(place * span_rows, (2 if order else 1) * span_rows)
        result = dot3(planes[0, span, :], planes[1, span, :], lead[0], lead[1])
        special = jnp.logical_and(
            lax.broadcasted_iota(jnp.int32, (span_rows, wide), 1) == drop, core == 0)
        if order:
            cr, sr = result[:span_rows, :wide], result[:span_rows, wide:]
            ci, si = result[span_rows:, :wide], result[span_rows:, wide:]
            values = [jnp.where(special, cr, cr + si), jnp.where(special, ci, ci - sr),
                      jnp.where(special, sr, cr - si), jnp.where(special, si, ci + sr)]
        else:
            values = [result[:, :wide], jnp.where(special, 0.0, -result[:, wide:])]
        for k, value in enumerate(values):
            hi, lo = halves(value)
            spec[0, :, pl.ds((first + k) * wide, wide)] = hi
            spec[1, :, pl.ds((first + k) * wide, wide)] = lo

    loads[0].wait()
    for k in range(2):
        fold_copy(sib_core, k).wait_recv()
    for order in range(1, orders + 1, 2):
        unmix([order])
        spectrum(order - 1)
    unmix(list(range(2, orders + 1, 2)) + [0])
    for order in range(2, orders + 1, 2):
        spectrum(order - 1)
    spectrum(orders)
    loads[1].wait()
    for first, tiles, _ in groups:
        window = pl.ds(first * wide, tiles * wide)
        mixed[:, window] = dot3(column[0], column[1], spec[0, :, window], spec[1, :, window])

    special = jnp.logical_and(lax.broadcasted_iota(jnp.int32, (STEP, wide), 1) == drop, core == 0)

    def combine(side):
        def block(first, odd, second, top):
            here, below = pl.ds(odd * quarter + first, STEP), pl.ds(half + odd * quarter + first, STEP)
            upper, lower = pl.ds(first, STEP), pl.ds(quarter + first, STEP)
            row0 = None
            if top:
                row0 = lax.broadcasted_iota(jnp.int32, (STEP, wide), 0) == 0

            def pick(at_top, value):
                return jnp.where(row0, at_top, value) if top else value

            def signs(tile):
                re, im = pl.ds(tile * wide, wide), pl.ds((tile + 1) * wide, wide)
                cr, ci, sr, si = mixed[here, re], mixed[here, im], mixed[below, re], mixed[below, im]
                plus = (pick(cr, cr + si), pick(ci, ci - sr))
                minus = (pick(sr, cr - si), pick(si, ci + sr))
                return plus, minus

            slots = (0, 1, 2, 3) if second else (0, 1)
            sums = {slot: [None, None] for slot in slots}

            def add(slot, k, term):
                sums[slot][k] = term if sums[slot][k] is None else sums[slot][k] + term

            if side == 0:
                center = signs(4 * orders)
                for slot in slots:
                    a = alpha[side, slot, mid, here, :]
                    for k in range(2):
                        add(slot, k, a * center[slot % 2][k])
            for order in range(1, orders + 1):
                pos, neg = signs(4 * (order - 1)), signs(4 * (order - 1) + 2)
                direct, other = (pos, neg) if side == 0 else (neg, pos)
                partner = [[jnp.where(special, direct[s][k], other[s][k]) for k in range(2)] for s in range(2)]
                if top:
                    swap = [[pick(partner[s][k], partner[1 - s][k]) for k in range(2)] for s in range(2)]
                else:
                    swap = [partner[1], partner[0]]
                for slot in slots:
                    s = slot % 2
                    up, down = alpha[side, slot, mid + order, here, :], alpha[side, slot, mid - order, here, :]
                    add(slot, 0, up * direct[s][0] + down * swap[s][0])
                    add(slot, 1, up * direct[s][1] - down * swap[s][1])
            for a in range(2):
                def folded(s, k):
                    if not second:
                        return sums[s][k]
                    return sums[s][k] + sums[2 + s][k] if a == 0 else sums[s][k] - sums[2 + s][k]

                pr, pi, mr, mi = folded(0, 0), folded(0, 1), folded(1, 0), folded(1, 1)
                low_top = (mr, mi) if a == 0 else (mi, -mr)
                values = [(upper, 0, pick(pr, pr + mr)), (upper, 1, pick(pi, pi + mi)),
                          (lower, 0, pick(low_top[0], mi - pi)), (lower, 1, pick(low_top[1], pr - mr))]
                for place, k, value in values:
                    hi, lo = halves(value)
                    coef[0, side, a, odd, place, pl.ds(k * wide, wide)] = hi
                    coef[1, side, a, odd, place, pl.ds(k * wide, wide)] = lo

        block(0, 0, True, True)
        blocks(block, False, True)

    flip = jnp.where(chip == 0, 1.0, -1.0)

    def to_rows(side, a):
        even, odd = [dot3(inverse[0, a, q], inverse[1, a, q], coef[0, side, a, q], coef[1, side, a, q])
                     for q in range(2)]
        odd = odd * flip
        return even + odd, even - odd

    def keep_near(side, a, value):
        first, second = value[:rows], value[rows:]
        near[core, side, a] = jnp.where(core == 0, first, second)
        near_send[side, a] = jnp.where(core == 0, second, first)
        near_copy(core, side, a).start()

    def a_copy(c, kc, slot_chip, slot_core, a):
        return pltpu.make_async_remote_copy(
            src_ref=send_a.at[c, a, pl.ds(kc * rows, rows), :], dst_ref=recv_a.at[slot_chip, slot_core, a],
            send_sem=a_ss.at[c, kc, a], recv_sem=a_rs.at[slot_chip, slot_core, a],
            device_id={"row": c * CORES + kc}, device_id_type=MESH)

    def b_copy(c, kc, slot_chip, slot_core, a):
        return pltpu.make_async_remote_copy(
            src_ref=send_b.at[c, kc, a], dst_ref=recv_b.at[slot_chip, slot_core, a],
            send_sem=b_ss.at[c, kc, a], recv_sem=b_rs.at[slot_chip, slot_core, a],
            device_id={"row": c * CORES + kc}, device_id_type=MESH)

    def near_copy(slot_core, side, a):
        return pltpu.make_async_remote_copy(
            src_ref=near_send.at[side, a], dst_ref=near.at[slot_core, side, a],
            send_sem=near_ss.at[side, a], recv_sem=near_rs.at[side, a],
            device_id={"row": sibling}, device_id_type=MESH)

    combine(0)
    loads[2].wait()
    for c in far_chips:
        for a in range(2):
            own_rows, far_rows = to_rows(0, a)
            send_a[c, a] = far_rows
            for kc in range(CORES):
                a_copy(c, kc, chip, core, a).start()
            keep_near(0, a, own_rows)

    make_alpha(1)
    combine(1)
    packed = send_b.shape[3]
    tail_rows = rows - packed
    lane_t = lax.broadcasted_iota(jnp.int32, (tail_rows, wide), 1)
    for c in far_chips:
        for a in range(2):
            own_rows, far_rows = to_rows(1, a)
            for kc in range(CORES):
                for k in range(2):
                    piece = far_rows[kc * rows:(kc + 1) * rows, k * wide:(k + 1) * wide]
                    tail = piece[packed:]
                    lanes = pl.ds(k * wide, wide)
                    send_b[c, kc, a, :, lanes] = piece[:packed]
                    for i, at in enumerate((0, packed - tail_rows)):
                        send_b[c, kc, a, pl.ds(at, tail_rows), lanes] = jnp.where(
                            lane_t < drop, pltpu.roll(tail, wide - drop * (i + 1), 1), piece[at:at + tail_rows])
                b_copy(c, kc, chip, core, a).start()
            keep_near(1, a, own_rows)

    loads[3].wait()
    chunk = 256
    for side in range(2):
        for a in range(2):
            near_copy(sib_core, side, a).wait_recv()

    def finish(a, side, pieces, write):
        split = [halves(piece) for piece in pieces]
        for x in range(0, pixels, chunk):
            span = pl.ds(x, chunk)
            even, odd = [dot3(hi, lo, last[0, k, side, :, span], last[1, k, side, :, span])
                         for k, (hi, lo) in enumerate(split)]
            write(a, x, even + odd)
            write(a, pixels + x, even - odd)

    def write_part(a, x, value):
        part[a, :, pl.ds(x, chunk)] = value

    def write_out(a, x, value):
        value = value + part[a, :, pl.ds(x, chunk)]
        for k in range(chunk // 128):
            tile = x // 128 + k
            woven[tile, pl.ds(a, rows, stride=2), :] = value[:, k * 128:(k + 1) * 128]
            if a:
                out[:, pl.ds(tile * 128, 128)] = woven[tile]

    for a in range(2):
        pieces = []
        for k in range(CORES):
            value = near[k, 0, a]
            for c in far_chips:
                a_copy(c, k, c, k, a).wait_recv()
                value = value + recv_a[c, k, a]
            pieces.append(value)
        finish(a, 0, pieces, write_part)

    def unpacked(c, k, a):
        sides = []
        for q in range(2):
            lanes = pl.ds(q * wide, wide)
            value = recv_b[c, k, a, :, lanes]
            first, second = value[:tail_rows], value[packed - tail_rows:]
            tail = jnp.where(lane_t < 2 * drop, pltpu.roll(first, drop, 1), pltpu.roll(second, 2 * drop, 1))
            sides.append(jnp.concatenate([value, tail], axis=0))
        return jnp.concatenate(sides, axis=1)

    for a in range(2):
        pieces = []
        for k in range(CORES):
            value = near[k, 1, a]
            for c in far_chips:
                b_copy(c, k, c, k, a).wait_recv()
                value = value + unpacked(c, k, a)
            pieces.append(value)
        finish(a, 1, pieces, write_out)

    for peer in others:
        tot_copy(peer, me).wait_send()
    for k in range(2):
        fold_copy(core, k).wait_send()
    for a in range(2):
        for side in range(2):
            near_copy(core, side, a).wait_send()
        for c in far_chips:
            for kc in range(CORES):
                a_copy(c, kc, chip, core, a).wait_send()
                b_copy(c, kc, chip, core, a).wait_send()


def solution(mesh):
    count = mesh.shape["row"]

    def per_device(frames, phase_offset, order_gain, band_shift):
        phases, rows, pixels = frames.shape[1:]
        chips = count // CORES
        assert chips == 2 and CORES == 2
        half = pixels // 2
        wide = half // CORES
        tiles = 4 * (phases // 2) + 2
        packed = -(-2 * rows // 24) * 8
        assert 2 * (rows - packed) <= packed
        lead, column, inverse, last = tables(pixels, count)
        vmem = pl.BlockSpec(memory_space=pltpu.VMEM)
        hbm = pl.BlockSpec(memory_space=pl.ANY)
        bf16, f32 = jnp.bfloat16, jnp.float32
        dma = pltpu.SemaphoreType.DMA
        return pl.pallas_call(
            functools.partial(kernel, count, otf_polynomial()),
            out_shape=pltpu.VMEM((2 * rows, 2 * pixels), f32),
            in_specs=[hbm] * 8,
            out_specs=vmem,
            scratch_shapes=[
                pltpu.SMEM(phase_offset.shape, f32),
                pltpu.SMEM(order_gain.shape, f32),
                pltpu.SMEM(band_shift.shape, jnp.int32),
                pltpu.VMEM((phases, rows, pixels), bf16),
                pltpu.VMEM((2, half, 2 * wide), bf16),
                pltpu.VMEM((2, pixels, CORES * rows), bf16),
                pltpu.VMEM(inverse.shape, bf16),
                pltpu.VMEM(last.shape, bf16),
                pltpu.VMEM((8, 128), f32),
                pltpu.VMEM((count, 8, 128), f32),
                pltpu.VMEM((2, phases, CORES * rows, half), f32),
                pltpu.VMEM((phases // 2, 2, CORES * rows, half), f32),
                pltpu.VMEM((2, phases * CORES * rows, half), bf16),
                pltpu.VMEM((2, CORES * rows, tiles * wide), bf16),
                pltpu.VMEM((pixels, tiles * wide), f32),
                pltpu.VMEM((2, 4, phases, half, wide), f32),
                pltpu.VMEM((2, 2, 2, 2, half, 2 * wide), bf16),
                pltpu.VMEM((2, 2, rows, 2 * wide), f32),
                pltpu.VMEM((CORES, 2, 2, rows, 2 * wide), f32),
                pltpu.VMEM((chips, 2, CORES * rows, 2 * wide), f32),
                pltpu.VMEM((chips, CORES, 2, rows, 2 * wide), f32),
                pltpu.VMEM((chips, CORES, 2, packed, 2 * wide), f32),
                pltpu.VMEM((chips, CORES, 2, packed, 2 * wide), f32),
                pltpu.VMEM((2, rows, 2 * pixels), f32),
                pltpu.VMEM((2 * pixels // 128, 2 * rows, 128), f32),
                dma((3,)), dma((phases,)), dma((4,)),
                dma((count,)), dma((count,)),
                dma((2,)), dma((2,)),
                dma((2, 2)), dma((2, 2)),
                dma((chips, CORES, 2)), dma((chips, CORES, 2)),
                dma((chips, CORES, 2)), dma((chips, CORES, 2)),
            ],
            compiler_params=pltpu.CompilerParams(
                collective_id=0, has_side_effects=True, vmem_limit_bytes=60000000
            ),
        )(frames, phase_offset, order_gain, band_shift,
          jnp.asarray(lead), jnp.asarray(column), jnp.asarray(inverse), jnp.asarray(last))

    in_specs = (P("fov", None, "row", None), P("fov"), P("fov", None), P("fov", None))
    return jax.shard_map(
        per_device, mesh=mesh, in_specs=in_specs, out_specs=P(("fov", "row"), None), check_vma=False
    )
```

```python
import functools
import math

import jax
import jax.numpy as jnp
import numpy as np
from jax import lax
from jax.experimental import pallas as pl
from jax.experimental.pallas import tpu as pltpu
from jax.sharding import PartitionSpec as P

MESH = pl.DeviceIdType.MESH
wiener = 0.1
gain_out = 8.0
cut_share = 0.45
CORES = 2
STEP = 16


def max_shift(pixels):
    return 3 * pixels // 16


def split_table(table):
    high = table.astype(np.float32).astype(jnp.bfloat16)
    low = (table - high.astype(np.float64)).astype(np.float32).astype(jnp.bfloat16)
    return np.stack([high, low])


def cos_sin(points, freqs, length):
    angle = 2.0 * math.pi * ((points[:, None] * freqs[None, :]) % length) / length
    return np.cos(angle), np.sin(angle)


def limits(pixels, orders):
    reach = [math.ceil((pixels - cut_share * pixels - k * max_shift(pixels)) / CORES) - 1 for k in (orders - 1, orders)]
    return reach[0], reach[1]


def lane_order(wide, drop):
    return np.concatenate([np.arange(1, drop + 1), [0], np.arange(drop + 1, wide)])


def tables(pixels, count, orders):
    half = pixels // 2
    wide = half // CORES
    chips = count // CORES
    drop, first = limits(pixels, orders)
    points = np.arange(pixels)
    freqs = np.arange(half)
    alternate = 1.0 - 2.0 * (points % 2)
    cos_f, sin_f = cos_sin(points, freqs, pixels)
    sin_f[:, 0] = alternate
    parities = [np.arange(q, half, 2) for q in range(2)]
    order = np.concatenate(parities)
    column = np.concatenate([cos_f[:, order], sin_f[:, order]], axis=1).T
    column = column.reshape(pixels, chips, pixels // chips).transpose(1, 0, 2)
    inverse = []
    for odd in range(2):
        cos_i, sin_i = cos_sin(2 * points[:half] + odd, freqs, 2 * pixels)
        sin_i[:, 0] = alternate[:half]
        inverse.append(np.stack([np.concatenate([cos_i[:, q], sin_i[:, q]], axis=1) for q in parities]))
    inverse = np.stack(inverse)
    lead, last = [], []
    places = np.arange(pixels)
    for core in range(CORES):
        own = CORES * lane_order(wide, drop) + core
        lead.append(np.concatenate([cos_f[:half, own], sin_f[:half, own]], axis=1))
        near_cos, near_sin = cos_sin(places, own, 2 * pixels)
        share = np.where(own == 0, 1.0, 2.0)
        near = np.concatenate([(near_cos * share).T, (-near_sin * share).T])
        mirror = np.where(own == 0, half, pixels - own)
        assert (pixels - own[:drop]).min() > cut_share * pixels + (orders - 1) * max_shift(pixels)
        assert (pixels - own[:first]).min() > cut_share * pixels + orders * max_shift(pixels)
        far_cos, far_sin = cos_sin(places, mirror, 2 * pixels)
        far = np.concatenate([(far_cos * 2.0).T, (-far_sin * 2.0).T])
        last.append(np.stack([near, far]))
    return tuple(split_table(t) for t in (np.stack(lead), column, inverse, np.stack(last)))


def otf_polynomial():
    nodes = 0.5 + 0.5 * np.cos(math.pi * (np.arange(64) + 0.5) / 64)
    nodes = np.minimum(nodes, 0.9985)
    values = 2 / math.pi * (np.arccos(nodes) - nodes * np.sqrt(1 - nodes * nodes)) / (1 - nodes) ** 1.5
    fit = np.polynomial.chebyshev.Chebyshev.fit(nodes, values, 6, domain=[0, 1])
    poly = fit.convert(kind=np.polynomial.Polynomial).coef
    return [float(c) for c in poly[::-1]]


def halves(value):
    high = value.astype(jnp.bfloat16)
    return high, (value - high.astype(jnp.float32)).astype(jnp.bfloat16)


def dot(left, right):
    return jnp.dot(left, right, preferred_element_type=jnp.float32)


def dot3(left_hi, left_lo, right_hi, right_lo):
    return dot(left_hi, right_hi) + (dot(left_hi, right_lo) + dot(left_lo, right_hi))


def kernel(count, poly, frames_h, offset_h, gain_h, shift_h, lead_h, column_h, inverse_h, last_h, out,
           offset, gain, shift, frames, lead, column, inverse, last, tot_send, tot, folds, ramps, planes, spec, mixed, outer, outer_send, outer_recv, mixed_outer, alpha, coef,
           near_send, near, send_a, recv_a, send_b, recv_b, part, woven,
           outer_ss, outer_rs, small_sem, frame_sem, table_sem, tot_ss, tot_rs, fold_ss, fold_rs, near_ss, near_rs, a_ss, a_rs, b_ss, b_rs):
    me = lax.axis_index("row")
    chips = count // CORES
    chip, core = me // CORES, me % CORES
    sib_core = 1 - core
    phases, rows, pixels = frames.shape
    half = pixels // 2
    wide = half // CORES
    orders = phases // 2
    drop, first_outer = limits(pixels, orders)
    turn_outer = drop - first_outer
    mid = phases // 2
    others = [lax.rem(me + step, count) for step in range(1, count)]
    far_chips = [lax.rem(chip + step, chips) for step in range(1, chips)]
    sibling = chip * CORES + sib_core

    barrier = pltpu.get_barrier_semaphore()
    for peer in others:
        pl.semaphore_signal(barrier, inc=1, device_id={"row": peer}, device_id_type=MESH)
    frame_loads = []
    for p in range(phases):
        frame_loads.append(pltpu.make_async_copy(frames_h.at[0, p], frames.at[p], frame_sem.at[p]))
        frame_loads[p].start()
    small = []
    for idx, (source, target) in enumerate(((offset_h, offset), (gain_h, gain), (shift_h, shift))):
        small.append(pltpu.make_async_copy(source, target, small_sem.at[idx]))
        small[idx].start()
    loads = []
    for idx, (source, target) in enumerate(
        ((lead_h.at[:, core], lead), (column_h, column), (inverse_h, inverse), (last_h, last))
    ):
        loads.append(pltpu.make_async_copy(source, target, table_sem.at[idx]))
    loads[0].start()

    mine = pl.ds(pl.multiple_of(core * rows, rows), rows)
    lane8 = lax.broadcasted_iota(jnp.int32, (8, 128), 1)
    total_part = jnp.zeros((8, 128), jnp.float32)
    for p in range(phases):
        frame_loads[p].wait()
        lower, upper = frames[p, :, :half].astype(jnp.float32), frames[p, :, half:].astype(jnp.float32)
        both = lower + upper
        folds[0, p, mine, :] = both
        folds[1, p, mine, :] = lower - upper
        s = jnp.sum(jnp.sum(both, axis=0, keepdims=True), axis=1, keepdims=True)
        total_part = total_part + jnp.where(lane8 == p, s, 0.0)
    tot_send[...] = total_part
    tot[me] = total_part
    pl.semaphore_wait(barrier, count - 1)

    def tot_copy(peer, slot):
        return pltpu.make_async_remote_copy(
            src_ref=tot_send, dst_ref=tot.at[slot], send_sem=tot_ss.at[peer], recv_sem=tot_rs.at[slot],
            device_id={"row": peer}, device_id_type=MESH)

    for peer in others:
        tot_copy(peer, me).start()

    def fold_copy(slot_core, k):
        place = pl.ds(pl.multiple_of(slot_core * rows, rows), rows)
        return pltpu.make_async_remote_copy(
            src_ref=folds.at[k, :, place], dst_ref=folds.at[k, :, place],
            send_sem=fold_ss.at[k], recv_sem=fold_rs.at[k],
            device_id={"row": sibling}, device_id_type=MESH)

    for k in range(2):
        fold_copy(core, k).start()
    for load in loads[1:]:
        load.start()

    for load in small:
        load.wait()
    shift_y, shift_x = shift[0, 0], shift[0, 1]
    inv_cut = 1.0 / (cut_share * pixels)
    scale_out = 0.5 * gain_out / (4.0 * pixels * pixels)
    gains = [gain[0, j] for j in range(phases)]
    squares = [g * g for g in gains]
    scaled = [g * scale_out for g in gains]
    reach = int(cut_share * pixels) + 1 + 2 * max_shift(pixels)
    single = max((pixels - reach) // 2 // STEP, 1)
    quarter = half // 2

    def blocks(block, few, many):
        for odd in range(2):
            def body(which, i, carry):
                block(pl.multiple_of(i * STEP, STEP), odd, which, False)
                return carry

            lax.fori_loop(1 - odd, single, functools.partial(body, few), 0)
            lax.fori_loop(single, quarter // STEP, functools.partial(body, many), 0)

    def own_freq(shape):
        lane = lax.broadcasted_iota(jnp.int32, shape, 1)
        place = jnp.where(lane < drop, lane + 1, jnp.where(lane == drop, 0, lane))
        return CORES * place + core

    def make_alpha(side):
        freq = own_freq((STEP, wide))
        if side:
            freq = jnp.where(freq == 0, half, pixels - freq)
        used = [j for j in range(phases) if not (side and j == mid)]
        sq_xs = {}
        for j in used:
            fx = (freq - (j - mid) * shift_x).astype(jnp.float32) * inv_cut
            sq_xs[j] = fx * fx + 1e-30
        offs = {j: ((j - mid) * shift_y).astype(jnp.float32) * inv_cut for j in used}

        def block(first, odd, slots, top):
            row = 2 * (first + lax.broadcasted_iota(jnp.int32, (STEP, wide), 0)) + odd
            here = pl.ds(odd * quarter + first, STEP)
            for slot in slots:
                big_y = row if slot % 2 == 0 else -row
                if top and slot % 2:
                    big_y = jnp.where(row == 0, -half, big_y)
                if slot == 2:
                    big_y = big_y - pixels
                if slot == 3:
                    big_y = big_y + pixels
                unit_y = big_y.astype(jnp.float32) * inv_cut
                den = jnp.full((STEP, wide), wiener, jnp.float32)
                den_m = jnp.full((STEP, wide), wiener, jnp.float32)
                values = {}
                for j in used:
                    fy = unit_y - offs[j]
                    t = fy * fy + sq_xs[j]
                    r = t * lax.rsqrt(t)
                    u = jnp.maximum(1.0 - r, 1e-30)
                    v = u * lax.rsqrt(u)
                    acc = poly[0] * r + poly[1]
                    for c in poly[2:]:
                        acc = acc * r + c
                    value = acc * (u * v)
                    values[j] = value
                    sq = value * value
                    den = den + squares[j] * sq
                    den_m = den_m + squares[phases - 1 - j] * sq
                both = 1.0 / (den * den_m)
                inv, inv_m = den_m * both, den * both
                for j in used:
                    alpha[side, slot, j, here, :] = values[j] * (
                        scaled[j] * inv + scaled[phases - 1 - j] * inv_m)

        block(0, 0, (0, 1, 2, 3), True)
        blocks(block, (0, 1), (0, 1, 2, 3))

    turn = 2.0 * math.pi / pixels

    def ramp(points, step):
        arg = ((points * step) & (pixels - 1)).astype(jnp.float32) * turn
        return jnp.cos(arg), jnp.sin(arg)

    def times(left, right):
        return left[0] * right[0] - left[1] * right[1], left[0] * right[1] + left[1] * right[0]

    row8 = lax.broadcasted_iota(jnp.int32, (8, 128), 0) + chip * (CORES * rows)
    wave_x = [ramp(lane8 + 128 * k, shift_x) for k in range(half // 128)]
    base = ramp(row8, shift_y)
    leap = ramp(jnp.full((8, 128), 8, jnp.int32), shift_y)
    pieces = [base]
    for k in range(1, CORES * rows // 8):
        pieces.append(times(pieces[-1], leap))
    wave_y = tuple(jnp.concatenate([q[k] for q in pieces], axis=0) for k in range(2))
    start = jnp.full((8, 128), offset[0], jnp.float32)
    wave_x = [times(w, (jnp.cos(start), -jnp.sin(start))) for w in wave_x]
    for k in range(half // 128):
        turned = times(wave_y, (wave_x[k][0][:1], wave_x[k][1][:1]))
        value = turned
        for order in range(orders):
            if order:
                value = times(value, turned)
            for q in range(2):
                ramps[order, q, :, pl.ds(k * 128, 128)] = value[q]

    make_alpha(0)

    for peer in others:
        tot_copy(peer, peer).wait_recv()
    total = tot[0]
    for d in range(1, count):
        total = total + tot[d]
    level = jnp.where(lane8 < phases, float(pixels * pixels), 0.0) / jnp.where(lane8 < phases, total, 1.0)
    level = level / phases

    groups = [(4 * g, 4, g + 1) for g in range(orders)] + [(4 * orders, 2, 0)]

    span_rows = CORES * rows

    def scaled_folds(which, rows_at, lanes_at):
        return [level[:1, p:p + 1] * folds[which, p, rows_at, lanes_at] for p in range(phases)]

    def modulated(order, values, rows_at, lanes_at):
        re, im = values[0], None
        for q in range(1, mid + 1):
            theta = 2.0 * math.pi * order * q / phases
            re = re + math.cos(theta) * (values[q] + values[phases - q])
            term = -math.sin(theta) * (values[q] - values[phases - q])
            im = term if im is None else im + term
        return times((re, im), [ramps[order - 1, k, rows_at, lanes_at] for k in range(2)])

    swapped = core + (shift_x & 1) * (1 - 2 * core)

    def unmix(wanted):
        which = swapped if wanted[0] % 2 else core
        for r in range(0, span_rows, STEP):
            for x in range(0, half, 128):
                rows_at, lanes_at = pl.ds(r, STEP), pl.ds(x, 128)
                values = scaled_folds(which, rows_at, lanes_at)
                for order in wanted:
                    if order:
                        made = modulated(order, values, rows_at, lanes_at)
                    else:
                        made = [functools.reduce(lambda a, b: a + b, values)]
                    for k, value in enumerate(made):
                        hi, lo = halves(value)
                        place = 2 * (order - 1) * span_rows + 2 * r + k * STEP if order else 2 * orders * span_rows + r
                        planes[0, pl.ds(place, STEP), lanes_at] = hi
                        planes[1, pl.ds(place, STEP), lanes_at] = lo

    forward = shift_x >= 0

    def outer_copy(c, slot_chip):
        return pltpu.make_async_remote_copy(
            src_ref=outer_send, dst_ref=outer_recv.at[slot_chip],
            send_sem=outer_ss.at[c], recv_sem=outer_rs.at[slot_chip],
            device_id={"row": c * CORES + core}, device_id_type=MESH)

    def spectrum(g):
        first, tiles, order = groups[g]
        place = 2 * (order - 1) if order else 2 * orders
        span = pl.ds(place * span_rows, (2 if order else 1) * span_rows)
        result = dot3(planes[0, span, :], planes[1, span, :], lead[0], lead[1])
        special = jnp.logical_and(lax.broadcasted_iota(jnp.int32, (STEP, wide), 1) == drop, core == 0)
        for r in range(0, span_rows, STEP):
            if order:
                re, im = result[2 * r:2 * r + STEP], result[2 * r + STEP:2 * r + 2 * STEP]
                cr, sr, ci, si = re[:, :wide], re[:, wide:], im[:, :wide], im[:, wide:]
                values = [jnp.where(special, cr, cr + si), jnp.where(special, ci, ci - sr),
                          jnp.where(special, sr, cr - si), jnp.where(special, si, ci + sr)]
            else:
                re = result[r:r + STEP]
                values = [re[:, :wide], jnp.where(special, 0.0, -re[:, wide:])]
            for k, value in enumerate(values):
                hi, lo = halves(value)
                spec[0, pl.ds(r, STEP), pl.ds((first + k) * wide, wide)] = hi
                spec[1, pl.ds(r, STEP), pl.ds((first + k) * wide, wide)] = lo
            if order == orders:
                outer_re = jnp.where(forward, values[2], values[0])
                outer_im = jnp.where(forward, values[3], -values[1])
                outer[pl.ds(r, STEP), pl.ds(0, wide)] = outer_re
                outer[pl.ds(r, STEP), pl.ds(wide, wide)] = outer_im
                lane = lax.broadcasted_iota(jnp.int32, (STEP, wide), 1)
                here = jnp.logical_and(lane >= first_outer, lane < drop)
                outer_send[pl.ds(r, STEP), :] = jnp.where(here, outer_re, pltpu.roll(outer_im, turn_outer, 1))

    loads[0].wait()
    for k in range(2):
        fold_copy(sib_core, k).wait_recv()
    for order in range(1, orders + 1, 2):
        unmix([order])
        spectrum(order - 1)
    unmix(list(range(2, orders + 1, 2)) + [0])
    for order in range(2, orders + 1, 2):
        spectrum(order - 1)
    for c in far_chips:
        outer_copy(c, chip).start()
    spectrum(orders)
    loads[1].wait()
    for first, tiles, _ in groups:
        window = pl.ds(first * wide, tiles * wide)
        mixed[:, window] = dot3(column[0, chip], column[1, chip], spec[0, :, window], spec[1, :, window])

    special = jnp.logical_and(lax.broadcasted_iota(jnp.int32, (STEP, wide), 1) == drop, core == 0)

    outer_lanes = lax.broadcasted_iota(jnp.int32, (STEP, wide), 1) < drop

    def combine(side):
        def block(first, odd, second, top):
            here, below = pl.ds(odd * quarter + first, STEP), pl.ds(half + odd * quarter + first, STEP)
            upper, lower = pl.ds(first, STEP), pl.ds(quarter + first, STEP)
            row0 = None
            if top:
                row0 = lax.broadcasted_iota(jnp.int32, (STEP, wide), 0) == 0

            def pick(at_top, value):
                return jnp.where(row0, at_top, value) if top else value

            def signs(tile, source=mixed):
                re, im = pl.ds(tile * wide, wide), pl.ds((tile + 1) * wide, wide)
                cr, ci, sr, si = source[here, re], source[here, im], source[below, re], source[below, im]
                plus = (pick(cr, cr + si), pick(ci, ci - sr))
                minus = (pick(sr, cr - si), pick(si, ci + sr))
                return plus, minus

            slots = (0, 1, 2, 3) if second else (0, 1)
            sums = {slot: [None, None] for slot in slots}

            def add(slot, k, term):
                sums[slot][k] = term if sums[slot][k] is None else sums[slot][k] + term

            if side == 0:
                center = signs(4 * orders)
                for slot in slots:
                    a = alpha[side, slot, mid, here, :]
                    for k in range(2):
                        add(slot, k, a * center[slot % 2][k])
            for order in range(1, orders + 1):
                pos, neg = signs(4 * (order - 1)), signs(4 * (order - 1) + 2)
                direct, other = (pos, neg) if side == 0 else (neg, pos)
                partner = [[jnp.where(special, direct[s][k], other[s][k]) for k in range(2)] for s in range(2)]
                if top:
                    swap = [[pick(partner[s][k], partner[1 - s][k]) for k in range(2)] for s in range(2)]
                else:
                    swap = [partner[1], partner[0]]
                for slot in slots:
                    s = slot % 2
                    up, down = alpha[side, slot, mid + order, here, :], alpha[side, slot, mid - order, here, :]
                    add(slot, 0, up * direct[s][0] + down * swap[s][0])
                    add(slot, 1, up * direct[s][1] - down * swap[s][1])
            if side:
                single_order = signs(0, mixed_outer)
                for slot in slots:
                    weight = jnp.where(forward, alpha[side, slot, mid + orders, here, :], alpha[side, slot, mid - orders, here, :])
                    for k in range(2):
                        sums[slot][k] = jnp.where(outer_lanes, weight * single_order[slot % 2][k], sums[slot][k])
            for a in range(2):
                def folded(s, k):
                    if not second:
                        return sums[s][k]
                    return sums[s][k] + sums[2 + s][k] if a == 0 else sums[s][k] - sums[2 + s][k]

                pr, pi, mr, mi = folded(0, 0), folded(0, 1), folded(1, 0), folded(1, 1)
                low_top = (mr, mi) if a == 0 else (mi, -mr)
                values = [(upper, 0, pick(pr, pr + mr)), (upper, 1, pick(pi, pi + mi)),
                          (lower, 0, pick(low_top[0], mi - pi)), (lower, 1, pick(low_top[1], pr - mr))]
                for place, k, value in values:
                    hi, lo = halves(value)
                    coef[0, side, a, odd, place, pl.ds(k * wide, wide)] = hi
                    coef[1, side, a, odd, place, pl.ds(k * wide, wide)] = lo

        block(0, 0, True, True)
        blocks(block, False, True)

    flip = jnp.where(chip == 0, 1.0, -1.0)

    def to_rows(side, a):
        even, odd = [dot3(inverse[0, a, q], inverse[1, a, q], coef[0, side, a, q], coef[1, side, a, q])
                     for q in range(2)]
        odd = odd * flip
        return even + odd, even - odd

    def keep_near(side, a, value):
        first, second = value[:rows], value[rows:]
        near[core, side, a] = jnp.where(core == 0, first, second)
        near_send[side, a] = jnp.where(core == 0, second, first)
        near_copy(core, side, a).start()

    def a_copy(c, kc, slot_chip, slot_core, a):
        return pltpu.make_async_remote_copy(
            src_ref=send_a.at[c, a, pl.ds(pl.multiple_of(kc * rows, rows), rows), :], dst_ref=recv_a.at[slot_chip, slot_core, a],
            send_sem=a_ss.at[c, kc, a], recv_sem=a_rs.at[slot_chip, slot_core, a],
            device_id={"row": c * CORES + kc}, device_id_type=MESH)

    def b_copy(c, kc, slot_chip, slot_core, a):
        return pltpu.make_async_remote_copy(
            src_ref=send_b.at[c, kc, a], dst_ref=recv_b.at[slot_chip, slot_core, a],
            send_sem=b_ss.at[c, kc, a], recv_sem=b_rs.at[slot_chip, slot_core, a],
            device_id={"row": c * CORES + kc}, device_id_type=MESH)

    def near_copy(slot_core, side, a):
        return pltpu.make_async_remote_copy(
            src_ref=near_send.at[side, a], dst_ref=near.at[slot_core, side, a],
            send_sem=near_ss.at[side, a], recv_sem=near_rs.at[side, a],
            device_id={"row": sibling}, device_id_type=MESH)

    combine(0)
    loads[2].wait()
    for c in far_chips:
        for a in range(2):
            own_rows, far_rows = to_rows(0, a)
            send_a[c, a] = far_rows
            for kc in (core, sib_core):
                a_copy(c, kc, chip, core, a).start()
            keep_near(0, a, own_rows)

    make_alpha(1)
    hi, lo = halves(outer[...])
    mixed_outer[...] = dot3(column[0, chip], column[1, chip], hi, lo)
    for c in far_chips:
        outer_copy(c, c).wait_recv()
        re = outer_recv[c]
        hi, lo = halves(jnp.concatenate([re, pltpu.roll(re, wide - turn_outer, 1)], axis=1))
        mixed_outer[...] += dot3(column[0, c], column[1, c], hi, lo)
    combine(1)
    packed = send_b.shape[3]
    tail_rows = (rows - packed) // 2
    kept = wide - drop
    lane_t = lax.broadcasted_iota(jnp.int32, (tail_rows, wide), 1)
    kept_lanes = lax.broadcasted_iota(jnp.int32, (rows, wide), 1) >= drop
    for c in far_chips:
        for a in range(2):
            own_rows, far_rows = to_rows(1, a)
            for kc in range(CORES):
                for k in range(2):
                    piece = far_rows[kc * rows:(kc + 1) * rows, k * wide:(k + 1) * wide]
                    lanes = pl.ds(k * wide, wide)
                    second, third = piece[packed:packed + tail_rows], piece[packed + tail_rows:]
                    send_b[c, kc, a, :, lanes] = piece[:packed]
                    send_b[c, kc, a, pl.ds(0, tail_rows), lanes] = jnp.where(
                        lane_t >= drop, piece[:tail_rows],
                        jnp.where(lane_t >= drop - kept, pltpu.roll(second, wide - kept, 1),
                                  pltpu.roll(third, wide - 2 * kept, 1)))
            for kc in (core, sib_core):
                b_copy(c, kc, chip, core, a).start()
            keep_near(1, a, own_rows)

    loads[3].wait()
    chunk = 256
    for side in range(2):
        for a in range(2):
            near_copy(sib_core, side, a).wait_recv()

    def finish(a, side, pieces, write):
        split = [halves(piece) for piece in pieces]
        for x in range(0, pixels, chunk):
            span = pl.ds(x, chunk)
            even, odd = [dot3(hi, lo, last[0, k, side, :, span], last[1, k, side, :, span])
                         for k, (hi, lo) in enumerate(split)]
            write(a, x, even + odd)
            write(a, pixels + x, even - odd)

    def write_part(a, x, value):
        part[a, :, pl.ds(x, chunk)] = value

    for a in range(2):
        pieces = []
        for k in range(CORES):
            value = near[k, 0, a]
            for c in far_chips:
                a_copy(c, k, c, k, a).wait_recv()
                value = value + recv_a[c, k, a]
            pieces.append(value)
        finish(a, 0, pieces, write_part)

    def unpacked(c, k, a):
        sides = []
        for q in range(2):
            lanes = pl.ds(q * wide, wide)
            value = recv_b[c, k, a, :, lanes]
            first = value[:tail_rows]
            joined = jnp.concatenate([value, pltpu.roll(first, kept, 1), pltpu.roll(first, 2 * kept, 1)], axis=0)
            sides.append(jnp.where(kept_lanes, joined, 0.0))
        return jnp.concatenate(sides, axis=1)

    for a in range(2):
        for k in (core, sib_core):
            sign = jnp.where(k == 0, 1.0, -1.0)
            value = near[k, 1, a]
            for c in far_chips:
                b_copy(c, k, c, k, a).wait_recv()
                value = value + unpacked(c, k, a)
            hi, lo = halves(value)
            for x in range(0, pixels, chunk):
                span = pl.ds(x, chunk)
                value = dot3(hi, lo, last[0, k, 1, :, span], last[1, k, 1, :, span])
                for at, term in ((x, value), (pixels + x, sign * value)):
                    total = part[a, :, pl.ds(at, chunk)] + term
                    if k is core:
                        part[a, :, pl.ds(at, chunk)] = total
                        continue
                    for q in range(chunk // 128):
                        tile = at // 128 + q
                        woven[tile, pl.ds(a, rows, stride=2), :] = total[:, q * 128:(q + 1) * 128]
                        if a:
                            out[:, pl.ds(tile * 128, 128)] = woven[tile]

    for peer in others:
        tot_copy(peer, me).wait_send()
    for k in range(2):
        fold_copy(core, k).wait_send()
    for c in far_chips:
        outer_copy(c, chip).wait_send()
    for a in range(2):
        for side in range(2):
            near_copy(core, side, a).wait_send()
        for c in far_chips:
            for kc in range(CORES):
                a_copy(c, kc, chip, core, a).wait_send()
                b_copy(c, kc, chip, core, a).wait_send()


def solution(mesh):
    count = mesh.shape["row"]

    def per_device(frames, phase_offset, order_gain, band_shift):
        phases, rows, pixels = frames.shape[1:]
        chips = count // CORES
        assert chips == 2 and CORES == 2
        half = pixels // 2
        wide = half // CORES
        tiles = 4 * (phases // 2) + 2
        packed = -(-rows // 24) * 8
        orders = phases // 2
        drop, first_outer = limits(pixels, orders)
        assert rows - packed <= 2 * packed and 3 * (wide - drop) <= wide and 2 * (drop - first_outer) <= wide
        lead, column, inverse, last = tables(pixels, count, orders)
        vmem = pl.BlockSpec(memory_space=pltpu.VMEM)
        hbm = pl.BlockSpec(memory_space=pl.ANY)
        bf16, f32 = jnp.bfloat16, jnp.float32
        dma = pltpu.SemaphoreType.DMA
        return pl.pallas_call(
            functools.partial(kernel, count, otf_polynomial()),
            out_shape=pltpu.VMEM((2 * rows, 2 * pixels), f32),
            in_specs=[hbm] * 8,
            out_specs=vmem,
            scratch_shapes=[
                pltpu.SMEM(phase_offset.shape, f32),
                pltpu.SMEM(order_gain.shape, f32),
                pltpu.SMEM(band_shift.shape, jnp.int32),
                pltpu.VMEM((phases, rows, pixels), bf16),
                pltpu.VMEM((2, half, 2 * wide), bf16),
                pltpu.VMEM(column.shape, bf16),
                pltpu.VMEM(inverse.shape, bf16),
                pltpu.VMEM(last.shape, bf16),
                pltpu.VMEM((8, 128), f32),
                pltpu.VMEM((count, 8, 128), f32),
                pltpu.VMEM((2, phases, CORES * rows, half), f32),
                pltpu.VMEM((phases // 2, 2, CORES * rows, half), f32),
                pltpu.VMEM((2, phases * CORES * rows, half), bf16),
                pltpu.VMEM((2, CORES * rows, tiles * wide), bf16),
                pltpu.VMEM((pixels, tiles * wide), f32),
                pltpu.VMEM((CORES * rows, 2 * wide), f32),
                pltpu.VMEM((CORES * rows, wide), f32),
                pltpu.VMEM((chips, CORES * rows, wide), f32),
                pltpu.VMEM((pixels, 2 * wide), f32),
                pltpu.VMEM((2, 4, phases, half, wide), f32),
                pltpu.VMEM((2, 2, 2, 2, half, 2 * wide), bf16),
                pltpu.VMEM((2, 2, rows, 2 * wide), f32),
                pltpu.VMEM((CORES, 2, 2, rows, 2 * wide), f32),
                pltpu.VMEM((chips, 2, CORES * rows, 2 * wide), f32),
                pltpu.VMEM((chips, CORES, 2, rows, 2 * wide), f32),
                pltpu.VMEM((chips, CORES, 2, packed, 2 * wide), f32),
                pltpu.VMEM((chips, CORES, 2, packed, 2 * wide), f32),
                pltpu.VMEM((2, rows, 2 * pixels), f32),
                pltpu.VMEM((2 * pixels // 128, 2 * rows, 128), f32),
                dma((chips,)), dma((chips,)),
                dma((3,)), dma((phases,)), dma((4,)),
                dma((count,)), dma((count,)),
                dma((2,)), dma((2,)),
                dma((2, 2)), dma((2, 2)),
                dma((chips, CORES, 2)), dma((chips, CORES, 2)),
                dma((chips, CORES, 2)), dma((chips, CORES, 2)),
            ],
            compiler_params=pltpu.CompilerParams(
                collective_id=0, has_side_effects=True, vmem_limit_bytes=60000000
            ),
        )(frames, phase_offset, order_gain, band_shift,
          jnp.asarray(lead), jnp.asarray(column), jnp.asarray(inverse), jnp.asarray(last))

    in_specs = (P("fov", None, "row", None), P("fov"), P("fov", None), P("fov", None))
    return jax.shard_map(
        per_device, mesh=mesh, in_specs=in_specs, out_specs=P(("fov", "row"), None), check_vma=False
    )
```

```python
import functools
import math

import jax
import jax.numpy as jnp
import numpy as np
from jax import lax
from jax.experimental import pallas as pl
from jax.experimental.pallas import tpu as pltpu
from jax.sharding import PartitionSpec as P

MESH = pl.DeviceIdType.MESH
wiener = 0.1
gain_out = 8.0
cut_share = 0.45
CORES = 2
STEP = 16


def max_shift(pixels):
    return 3 * pixels // 16


def split_table(table):
    high = table.astype(np.float32).astype(jnp.bfloat16)
    low = (table - high.astype(np.float64)).astype(np.float32).astype(jnp.bfloat16)
    return np.stack([high, low])


def cos_sin(points, freqs, length):
    angle = 2.0 * math.pi * ((points[:, None] * freqs[None, :]) % length) / length
    return np.cos(angle), np.sin(angle)


def limits(pixels, orders):
    lone, first = [math.ceil((pixels - cut_share * pixels - k * max_shift(pixels)) / CORES) - 1
                   for k in (orders - 1, orders)]
    wide = pixels // 2 // CORES
    return max(lone, wide - wide // 4), lone, first


def lane_order(wide, drop):
    return np.concatenate([np.arange(1, drop + 1), [0], np.arange(drop + 1, wide)])


def tables(pixels, count, orders):
    half = pixels // 2
    wide = half // CORES
    chips = count // CORES
    drop, lone, first = limits(pixels, orders)
    points = np.arange(pixels)
    freqs = np.arange(half)
    alternate = 1.0 - 2.0 * (points % 2)
    cos_f, sin_f = cos_sin(points, freqs, pixels)
    sin_f[:, 0] = alternate
    parities = [np.arange(q, half, 2) for q in range(2)]
    order = np.concatenate(parities)
    column = np.concatenate([cos_f[:, order], sin_f[:, order]], axis=1).T
    column = column.reshape(pixels, chips, pixels // chips).transpose(1, 0, 2)
    inverse = []
    for odd in range(2):
        cos_i, sin_i = cos_sin(2 * points[:half] + odd, freqs, 2 * pixels)
        sin_i[:, 0] = alternate[:half]
        inverse.append(np.stack([np.concatenate([cos_i[:, q], sin_i[:, q]], axis=1) for q in parities]))
    inverse = np.stack(inverse)
    lead, last = [], []
    places = np.arange(pixels)
    for core in range(CORES):
        own = CORES * lane_order(wide, drop) + core
        lead.append(np.concatenate([cos_f[:half, own], sin_f[:half, own]], axis=1))
        near_cos, near_sin = cos_sin(places, own, 2 * pixels)
        share = np.where(own == 0, 1.0, 2.0)
        near = np.concatenate([(near_cos * share).T, (-near_sin * share).T])
        mirror = np.where(own == 0, half, pixels - own)
        assert (pixels - own[:lone]).min() > cut_share * pixels + (orders - 1) * max_shift(pixels)
        assert (pixels - own[:first]).min() > cut_share * pixels + orders * max_shift(pixels)
        far_cos, far_sin = cos_sin(places, mirror, 2 * pixels)
        far = np.concatenate([(far_cos * 2.0).T, (-far_sin * 2.0).T])
        last.append(np.stack([near, far]))
    return tuple(split_table(t) for t in (np.stack(lead), column, inverse, np.stack(last)))


def otf_polynomial():
    nodes = 0.5 + 0.5 * np.cos(math.pi * (np.arange(64) + 0.5) / 64)
    nodes = np.minimum(nodes, 0.9985)
    values = 2 / math.pi * (np.arccos(nodes) - nodes * np.sqrt(1 - nodes * nodes)) / (1 - nodes) ** 1.5
    fit = np.polynomial.chebyshev.Chebyshev.fit(nodes, values, 6, domain=[0, 1])
    poly = fit.convert(kind=np.polynomial.Polynomial).coef
    return [float(c) for c in poly[::-1]]


def halves(value):
    high = value.astype(jnp.bfloat16)
    return high, (value - high.astype(jnp.float32)).astype(jnp.bfloat16)


def dot(left, right):
    return jnp.dot(left, right, preferred_element_type=jnp.float32)


def dot3(left_hi, left_lo, right_hi, right_lo):
    return dot(left_hi, right_hi) + (dot(left_hi, right_lo) + dot(left_lo, right_hi))


def kernel(count, poly, frames_h, offset_h, gain_h, shift_h, lead_h, column_h, inverse_h, last_h, out,
           offset, gain, shift, frames, lead, column, inverse, last, tot_send, tot, folds, ramps, planes, spec, mixed, outer, outer_send, outer_recv, mixed_outer, alpha, coef,
           near_send, near, send_a, recv_a, send_b, recv_b, part, woven,
           outer_ss, outer_rs, small_sem, frame_sem, table_sem, tot_ss, tot_rs, fold_ss, fold_rs, near_ss, near_rs, a_ss, a_rs, b_ss, b_rs):
    me = lax.axis_index("row")
    chips = count // CORES
    chip, core = me // CORES, me % CORES
    sib_core = 1 - core
    phases, rows, pixels = frames.shape
    half = pixels // 2
    wide = half // CORES
    orders = phases // 2
    drop, lone, first_outer = limits(pixels, orders)
    turn_outer, pair = drop - first_outer, drop - lone
    mid = phases // 2
    others = [lax.rem(me + step, count) for step in range(1, count)]
    far_chips = [lax.rem(chip + step, chips) for step in range(1, chips)]
    sibling = chip * CORES + sib_core

    barrier = pltpu.get_barrier_semaphore()
    for peer in others:
        pl.semaphore_signal(barrier, inc=1, device_id={"row": peer}, device_id_type=MESH)
    frame_loads = []
    for p in range(phases):
        frame_loads.append(pltpu.make_async_copy(frames_h.at[0, p], frames.at[p], frame_sem.at[p]))
        frame_loads[p].start()
    small = []
    for idx, (source, target) in enumerate(((offset_h, offset), (gain_h, gain), (shift_h, shift))):
        small.append(pltpu.make_async_copy(source, target, small_sem.at[idx]))
        small[idx].start()
    loads = []
    for idx, (source, target) in enumerate(
        ((lead_h.at[:, core], lead), (column_h, column), (inverse_h, inverse), (last_h, last))
    ):
        loads.append(pltpu.make_async_copy(source, target, table_sem.at[idx]))
    loads[0].start()

    mine = pl.ds(pl.multiple_of(core * rows, rows), rows)
    lane8 = lax.broadcasted_iota(jnp.int32, (8, 128), 1)
    total_part = jnp.zeros((8, 128), jnp.float32)
    for p in range(phases):
        frame_loads[p].wait()
        lower, upper = frames[p, :, :half].astype(jnp.float32), frames[p, :, half:].astype(jnp.float32)
        both = lower + upper
        folds[0, p, mine, :] = both
        folds[1, p, mine, :] = lower - upper
        s = jnp.sum(jnp.sum(both, axis=0, keepdims=True), axis=1, keepdims=True)
        total_part = total_part + jnp.where(lane8 == p, s, 0.0)
    tot_send[...] = total_part
    tot[me] = total_part
    pl.semaphore_wait(barrier, count - 1)

    def tot_copy(peer, slot):
        return pltpu.make_async_remote_copy(
            src_ref=tot_send, dst_ref=tot.at[slot], send_sem=tot_ss.at[peer], recv_sem=tot_rs.at[slot],
            device_id={"row": peer}, device_id_type=MESH)

    for peer in others:
        tot_copy(peer, me).start()

    def fold_copy(slot_core, k):
        place = pl.ds(pl.multiple_of(slot_core * rows, rows), rows)
        return pltpu.make_async_remote_copy(
            src_ref=folds.at[k, :, place], dst_ref=folds.at[k, :, place],
            send_sem=fold_ss.at[k], recv_sem=fold_rs.at[k],
            device_id={"row": sibling}, device_id_type=MESH)

    for k in range(2):
        fold_copy(core, k).start()
    for load in loads[1:]:
        load.start()

    for load in small:
        load.wait()
    shift_y, shift_x = shift[0, 0], shift[0, 1]
    inv_cut = 1.0 / (cut_share * pixels)
    scale_out = 0.5 * gain_out / (4.0 * pixels * pixels)
    gains = [gain[0, j] for j in range(phases)]
    squares = [g * g for g in gains]
    scaled = [g * scale_out for g in gains]
    reach = int(cut_share * pixels) + 1 + 2 * max_shift(pixels)
    single = max((pixels - reach) // 2 // STEP, 1)
    quarter = half // 2

    def blocks(block, few, many):
        for odd in range(2):
            def body(which, i, carry):
                block(pl.multiple_of(i * STEP, STEP), odd, which, False)
                return carry

            lax.fori_loop(1 - odd, single, functools.partial(body, few), 0)
            lax.fori_loop(single, quarter // STEP, functools.partial(body, many), 0)

    def own_freq(shape):
        lane = lax.broadcasted_iota(jnp.int32, shape, 1)
        place = jnp.where(lane < drop, lane + 1, jnp.where(lane == drop, 0, lane))
        return CORES * place + core

    def make_alpha(side):
        freq = own_freq((STEP, wide))
        if side:
            freq = jnp.where(freq == 0, half, pixels - freq)
        used = [j for j in range(phases) if not (side and j == mid)]
        sq_xs = {}
        for j in used:
            fx = (freq - (j - mid) * shift_x).astype(jnp.float32) * inv_cut
            sq_xs[j] = fx * fx + 1e-30
        offs = {j: ((j - mid) * shift_y).astype(jnp.float32) * inv_cut for j in used}

        def block(first, odd, slots, top):
            row = 2 * (first + lax.broadcasted_iota(jnp.int32, (STEP, wide), 0)) + odd
            here = pl.ds(odd * quarter + first, STEP)
            for slot in slots:
                big_y = row if slot % 2 == 0 else -row
                if top and slot % 2:
                    big_y = jnp.where(row == 0, -half, big_y)
                if slot == 2:
                    big_y = big_y - pixels
                if slot == 3:
                    big_y = big_y + pixels
                unit_y = big_y.astype(jnp.float32) * inv_cut
                den = jnp.full((STEP, wide), wiener, jnp.float32)
                den_m = jnp.full((STEP, wide), wiener, jnp.float32)
                values = {}
                for j in used:
                    fy = unit_y - offs[j]
                    t = fy * fy + sq_xs[j]
                    r = t * lax.rsqrt(t)
                    u = jnp.maximum(1.0 - r, 1e-30)
                    v = u * lax.rsqrt(u)
                    acc = poly[0] * r + poly[1]
                    for c in poly[2:]:
                        acc = acc * r + c
                    value = acc * (u * v)
                    values[j] = value
                    sq = value * value
                    den = den + squares[j] * sq
                    den_m = den_m + squares[phases - 1 - j] * sq
                both = 1.0 / (den * den_m)
                inv, inv_m = den_m * both, den * both
                for j in used:
                    alpha[side, slot, j, here, :] = values[j] * (
                        scaled[j] * inv + scaled[phases - 1 - j] * inv_m)

        block(0, 0, (0, 1, 2, 3), True)
        blocks(block, (0, 1), (0, 1, 2, 3))

    turn = 2.0 * math.pi / pixels

    def ramp(points, step):
        arg = ((points * step) & (pixels - 1)).astype(jnp.float32) * turn
        return jnp.cos(arg), jnp.sin(arg)

    def times(left, right):
        return left[0] * right[0] - left[1] * right[1], left[0] * right[1] + left[1] * right[0]

    row8 = lax.broadcasted_iota(jnp.int32, (8, 128), 0) + chip * (CORES * rows)
    wave_x = [ramp(lane8 + 128 * k, shift_x) for k in range(half // 128)]
    base = ramp(row8, shift_y)
    leap = ramp(jnp.full((8, 128), 8, jnp.int32), shift_y)
    pieces = [base]
    for k in range(1, CORES * rows // 8):
        pieces.append(times(pieces[-1], leap))
    wave_y = tuple(jnp.concatenate([q[k] for q in pieces], axis=0) for k in range(2))
    start = jnp.full((8, 128), offset[0], jnp.float32)
    wave_x = [times(w, (jnp.cos(start), -jnp.sin(start))) for w in wave_x]
    for k in range(half // 128):
        turned = times(wave_y, (wave_x[k][0][:1], wave_x[k][1][:1]))
        value = turned
        for order in range(orders):
            if order:
                value = times(value, turned)
            for q in range(2):
                ramps[order, q, :, pl.ds(k * 128, 128)] = value[q]

    make_alpha(0)

    for peer in others:
        tot_copy(peer, peer).wait_recv()
    total = tot[0]
    for d in range(1, count):
        total = total + tot[d]
    level = jnp.where(lane8 < phases, float(pixels * pixels), 0.0) / jnp.where(lane8 < phases, total, 1.0)
    level = level / phases

    groups = [(4 * g, 4, g + 1) for g in range(orders)] + [(4 * orders, 2, 0)]

    span_rows = CORES * rows

    def scaled_folds(which, rows_at, lanes_at):
        return [level[:1, p:p + 1] * folds[which, p, rows_at, lanes_at] for p in range(phases)]

    def modulated(order, values, rows_at, lanes_at):
        re, im = values[0], None
        for q in range(1, mid + 1):
            theta = 2.0 * math.pi * order * q / phases
            re = re + math.cos(theta) * (values[q] + values[phases - q])
            term = -math.sin(theta) * (values[q] - values[phases - q])
            im = term if im is None else im + term
        return times((re, im), [ramps[order - 1, k, rows_at, lanes_at] for k in range(2)])

    swapped = core + (shift_x & 1) * (1 - 2 * core)

    def unmix(wanted):
        which = swapped if wanted[0] % 2 else core
        for r in range(0, span_rows, STEP):
            for x in range(0, half, 128):
                rows_at, lanes_at = pl.ds(r, STEP), pl.ds(x, 128)
                values = scaled_folds(which, rows_at, lanes_at)
                for order in wanted:
                    if order:
                        made = modulated(order, values, rows_at, lanes_at)
                    else:
                        made = [functools.reduce(lambda a, b: a + b, values)]
                    for k, value in enumerate(made):
                        hi, lo = halves(value)
                        place = 2 * (order - 1) * span_rows + 2 * r + k * STEP if order else 2 * orders * span_rows + r
                        planes[0, pl.ds(place, STEP), lanes_at] = hi
                        planes[1, pl.ds(place, STEP), lanes_at] = lo

    forward = shift_x >= 0
    free = first_outer + 2 * turn_outer - wide

    def outer_copy(c, slot_chip):
        return pltpu.make_async_remote_copy(
            src_ref=outer_send, dst_ref=outer_recv.at[slot_chip],
            send_sem=outer_ss.at[c], recv_sem=outer_rs.at[slot_chip],
            device_id={"row": c * CORES + core}, device_id_type=MESH)

    def spectrum(g):
        first, tiles, order = groups[g]
        place = 2 * (order - 1) if order else 2 * orders
        span = pl.ds(place * span_rows, (2 if order else 1) * span_rows)
        result = dot3(planes[0, span, :], planes[1, span, :], lead[0], lead[1])
        special = jnp.logical_and(lax.broadcasted_iota(jnp.int32, (STEP, wide), 1) == drop, core == 0)
        for r in range(0, span_rows, STEP):
            if order:
                re, im = result[2 * r:2 * r + STEP], result[2 * r + STEP:2 * r + 2 * STEP]
                cr, sr, ci, si = re[:, :wide], re[:, wide:], im[:, :wide], im[:, wide:]
                values = [jnp.where(special, cr, cr + si), jnp.where(special, ci, ci - sr),
                          jnp.where(special, sr, cr - si), jnp.where(special, si, ci + sr)]
            else:
                re = result[r:r + STEP]
                values = [re[:, :wide], jnp.where(special, 0.0, -re[:, wide:])]
            for k, value in enumerate(values):
                hi, lo = halves(value)
                spec[0, pl.ds(r, STEP), pl.ds((first + k) * wide, wide)] = hi
                spec[1, pl.ds(r, STEP), pl.ds((first + k) * wide, wide)] = lo
            if order >= orders - 1:
                place = (orders - order) * 2 * wide
                outer_re = jnp.where(forward, values[2], values[0])
                outer_im = jnp.where(forward, values[3], -values[1])
                outer[pl.ds(r, STEP), pl.ds(place, wide)] = outer_re
                outer[pl.ds(r, STEP), pl.ds(place + wide, wide)] = outer_im
                lane = lax.broadcasted_iota(jnp.int32, (STEP, wide), 1)
                if order == orders:
                    here = jnp.logical_and(lane >= first_outer, lane < drop)
                    full = jnp.where(here, outer_re, pltpu.roll(outer_im, turn_outer, 1))
                    below = jnp.logical_and(lane >= free, lane < free + 2 * pair)
                    outer_send[pl.ds(r, STEP), :] = jnp.where(below, outer_send[pl.ds(r, STEP), :], full)
                else:
                    outer_send[pl.ds(r, STEP), :] = jnp.where(
                        lane < free + pair, pltpu.roll(outer_re, wide - (lone - free), 1),
                        pltpu.roll(outer_im, wide - (lone - free - pair), 1))

    loads[0].wait()
    for k in range(2):
        fold_copy(sib_core, k).wait_recv()
    for order in range(1, orders + 1, 2):
        unmix([order])
        spectrum(order - 1)
    unmix(list(range(2, orders + 1, 2)) + [0])
    for order in range(2, orders + 1, 2):
        spectrum(order - 1)
    for c in far_chips:
        outer_copy(c, chip).start()
    spectrum(orders)
    loads[1].wait()
    for first, tiles, _ in groups:
        window = pl.ds(first * wide, tiles * wide)
        mixed[:, window] = dot3(column[0, chip], column[1, chip], spec[0, :, window], spec[1, :, window])

    special = jnp.logical_and(lax.broadcasted_iota(jnp.int32, (STEP, wide), 1) == drop, core == 0)

    outer_lanes = lax.broadcasted_iota(jnp.int32, (STEP, wide), 1) < drop

    def combine(side):
        def block(first, odd, second, top):
            here, below = pl.ds(odd * quarter + first, STEP), pl.ds(half + odd * quarter + first, STEP)
            upper, lower = pl.ds(first, STEP), pl.ds(quarter + first, STEP)
            row0 = None
            if top:
                row0 = lax.broadcasted_iota(jnp.int32, (STEP, wide), 0) == 0

            def pick(at_top, value):
                return jnp.where(row0, at_top, value) if top else value

            def signs(tile, source=mixed):
                re, im = pl.ds(tile * wide, wide), pl.ds((tile + 1) * wide, wide)
                cr, ci, sr, si = source[here, re], source[here, im], source[below, re], source[below, im]
                plus = (pick(cr, cr + si), pick(ci, ci - sr))
                minus = (pick(sr, cr - si), pick(si, ci + sr))
                return plus, minus

            slots = (0, 1, 2, 3) if second else (0, 1)
            sums = {slot: [None, None] for slot in slots}

            def add(slot, k, term):
                sums[slot][k] = term if sums[slot][k] is None else sums[slot][k] + term

            if side == 0:
                center = signs(4 * orders)
                for slot in slots:
                    a = alpha[side, slot, mid, here, :]
                    for k in range(2):
                        add(slot, k, a * center[slot % 2][k])
            for order in range(1, orders + 1):
                pos, neg = signs(4 * (order - 1)), signs(4 * (order - 1) + 2)
                direct, other = (pos, neg) if side == 0 else (neg, pos)
                partner = [[jnp.where(special, direct[s][k], other[s][k]) for k in range(2)] for s in range(2)]
                if top:
                    swap = [[pick(partner[s][k], partner[1 - s][k]) for k in range(2)] for s in range(2)]
                else:
                    swap = [partner[1], partner[0]]
                for slot in slots:
                    s = slot % 2
                    up, down = alpha[side, slot, mid + order, here, :], alpha[side, slot, mid - order, here, :]
                    add(slot, 0, up * direct[s][0] + down * swap[s][0])
                    add(slot, 1, up * direct[s][1] - down * swap[s][1])
            if side:
                outer_parts = [(orders - q, signs(2 * q, mixed_outer)) for q in range(2)]
                for slot in slots:
                    weights = [jnp.where(forward, alpha[side, slot, mid + order, here, :],
                                         alpha[side, slot, mid - order, here, :]) for order, _ in outer_parts]
                    for k in range(2):
                        whole = weights[0] * outer_parts[0][1][slot % 2][k] + weights[1] * outer_parts[1][1][slot % 2][k]
                        sums[slot][k] = jnp.where(outer_lanes, whole, sums[slot][k])
            for a in range(2):
                def folded(s, k):
                    if not second:
                        return sums[s][k]
                    return sums[s][k] + sums[2 + s][k] if a == 0 else sums[s][k] - sums[2 + s][k]

                pr, pi, mr, mi = folded(0, 0), folded(0, 1), folded(1, 0), folded(1, 1)
                low_top = (mr, mi) if a == 0 else (mi, -mr)
                values = [(upper, 0, pick(pr, pr + mr)), (upper, 1, pick(pi, pi + mi)),
                          (lower, 0, pick(low_top[0], mi - pi)), (lower, 1, pick(low_top[1], pr - mr))]
                for place, k, value in values:
                    hi, lo = halves(value)
                    coef[0, side, a, odd, place, pl.ds(k * wide, wide)] = hi
                    coef[1, side, a, odd, place, pl.ds(k * wide, wide)] = lo

        block(0, 0, True, True)
        blocks(block, False, True)

    flip = jnp.where(chip == 0, 1.0, -1.0)

    def to_rows(side, a):
        even, odd = [dot3(inverse[0, a, q], inverse[1, a, q], coef[0, side, a, q], coef[1, side, a, q])
                     for q in range(2)]
        odd = odd * flip
        return even + odd, even - odd

    def keep_near(side, a, value):
        first, second = value[:rows], value[rows:]
        near[core, side, a] = jnp.where(core == 0, first, second)
        near_send[side, a] = jnp.where(core == 0, second, first)
        near_copy(core, side, a).start()

    def a_copy(c, kc, slot_chip, slot_core, a):
        return pltpu.make_async_remote_copy(
            src_ref=send_a.at[c, a, pl.ds(pl.multiple_of(kc * rows, rows), rows), :], dst_ref=recv_a.at[slot_chip, slot_core, a],
            send_sem=a_ss.at[c, kc, a], recv_sem=a_rs.at[slot_chip, slot_core, a],
            device_id={"row": c * CORES + kc}, device_id_type=MESH)

    def b_copy(c, kc, slot_chip, slot_core, a):
        return pltpu.make_async_remote_copy(
            src_ref=send_b.at[c, kc, a], dst_ref=recv_b.at[slot_chip, slot_core, a],
            send_sem=b_ss.at[c, kc, a], recv_sem=b_rs.at[slot_chip, slot_core, a],
            device_id={"row": c * CORES + kc}, device_id_type=MESH)

    def near_copy(slot_core, side, a):
        return pltpu.make_async_remote_copy(
            src_ref=near_send.at[side, a], dst_ref=near.at[slot_core, side, a],
            send_sem=near_ss.at[side, a], recv_sem=near_rs.at[side, a],
            device_id={"row": sibling}, device_id_type=MESH)

    combine(0)
    loads[2].wait()
    for c in far_chips:
        for a in range(2):
            own_rows, far_rows = to_rows(0, a)
            send_a[c, a] = far_rows
            for kc in (core, sib_core):
                a_copy(c, kc, chip, core, a).start()
            keep_near(0, a, own_rows)

    make_alpha(1)
    hi, lo = halves(outer[...])
    mixed_outer[...] = dot3(column[0, chip], column[1, chip], hi, lo)
    for c in far_chips:
        outer_copy(c, c).wait_recv()
        tile = outer_recv[c]
        hi, lo = halves(jnp.concatenate([tile, pltpu.roll(tile, wide - turn_outer, 1), pltpu.roll(tile, lone - free, 1),
                                         pltpu.roll(tile, lone - free - pair, 1)], axis=1))
        mixed_outer[...] += dot3(column[0, c], column[1, c], hi, lo)
    combine(1)
    packed = send_b.shape[3]
    shared = rows // packed
    kept = wide - drop
    lane_t = lax.broadcasted_iota(jnp.int32, (packed, wide), 1)
    kept_lanes = lax.broadcasted_iota(jnp.int32, (rows, wide), 1) >= drop
    for c in far_chips:
        for a in range(2):
            own_rows, far_rows = to_rows(1, a)
            for kc in range(CORES):
                for k in range(2):
                    piece = far_rows[kc * rows:(kc + 1) * rows, k * wide:(k + 1) * wide]
                    lanes = pl.ds(k * wide, wide)
                    value = piece[:packed]
                    for i in range(1, shared):
                        moved = pltpu.roll(piece[i * packed:(i + 1) * packed], wide - i * kept, 1)
                        value = jnp.where(lane_t < wide - i * kept, moved, value)
                    send_b[c, kc, a, :, lanes] = value
            for kc in (core, sib_core):
                b_copy(c, kc, chip, core, a).start()
            keep_near(1, a, own_rows)

    loads[3].wait()
    chunk = 256
    for side in range(2):
        for a in range(2):
            near_copy(sib_core, side, a).wait_recv()

    def finish(a, side, pieces, write):
        split = [halves(piece) for piece in pieces]
        for x in range(0, pixels, chunk):
            span = pl.ds(x, chunk)
            even, odd = [dot3(hi, lo, last[0, k, side, :, span], last[1, k, side, :, span])
                         for k, (hi, lo) in enumerate(split)]
            write(a, x, even + odd)
            write(a, pixels + x, even - odd)

    def write_part(a, x, value):
        part[a, :, pl.ds(x, chunk)] = value

    for a in range(2):
        pieces = []
        for k in range(CORES):
            value = near[k, 0, a]
            for c in far_chips:
                a_copy(c, k, c, k, a).wait_recv()
                value = value + recv_a[c, k, a]
            pieces.append(value)
        finish(a, 0, pieces, write_part)

    def unpacked(c, k, a):
        sides = []
        for q in range(2):
            lanes = pl.ds(q * wide, wide)
            value = recv_b[c, k, a, :, lanes]
            joined = jnp.concatenate([value] + [pltpu.roll(value, i * kept, 1) for i in range(1, shared)], axis=0)
            sides.append(jnp.where(kept_lanes, joined, 0.0))
        return jnp.concatenate(sides, axis=1)

    for a in range(2):
        for k in (core, sib_core):
            sign = jnp.where(k == 0, 1.0, -1.0)
            value = near[k, 1, a]
            for c in far_chips:
                b_copy(c, k, c, k, a).wait_recv()
                value = value + unpacked(c, k, a)
            hi, lo = halves(value)
            for x in range(0, pixels, chunk):
                span = pl.ds(x, chunk)
                value = dot3(hi, lo, last[0, k, 1, :, span], last[1, k, 1, :, span])
                for at, term in ((x, value), (pixels + x, sign * value)):
                    total = part[a, :, pl.ds(at, chunk)] + term
                    if k is core:
                        part[a, :, pl.ds(at, chunk)] = total
                        continue
                    for q in range(chunk // 128):
                        tile = at // 128 + q
                        woven[tile, pl.ds(a, rows, stride=2), :] = total[:, q * 128:(q + 1) * 128]
                        if a:
                            out[:, pl.ds(tile * 128, 128)] = woven[tile]

    for peer in others:
        tot_copy(peer, me).wait_send()
    for k in range(2):
        fold_copy(core, k).wait_send()
    for c in far_chips:
        outer_copy(c, chip).wait_send()
    for a in range(2):
        for side in range(2):
            near_copy(core, side, a).wait_send()
        for c in far_chips:
            for kc in range(CORES):
                a_copy(c, kc, chip, core, a).wait_send()
                b_copy(c, kc, chip, core, a).wait_send()


def solution(mesh):
    count = mesh.shape["row"]

    def per_device(frames, phase_offset, order_gain, band_shift):
        phases, rows, pixels = frames.shape[1:]
        chips = count // CORES
        assert chips == 2 and CORES == 2
        half = pixels // 2
        wide = half // CORES
        tiles = 4 * (phases // 2) + 2
        packed = rows // 4
        orders = phases // 2
        drop, lone, first = limits(pixels, orders)
        assert 4 * (wide - drop) <= wide and 2 * (drop - first) + 2 * (drop - lone) <= wide < 2 * drop
        lead, column, inverse, last = tables(pixels, count, orders)
        vmem = pl.BlockSpec(memory_space=pltpu.VMEM)
        hbm = pl.BlockSpec(memory_space=pl.ANY)
        bf16, f32 = jnp.bfloat16, jnp.float32
        dma = pltpu.SemaphoreType.DMA
        return pl.pallas_call(
            functools.partial(kernel, count, otf_polynomial()),
            out_shape=pltpu.VMEM((2 * rows, 2 * pixels), f32),
            in_specs=[hbm] * 8,
            out_specs=vmem,
            scratch_shapes=[
                pltpu.SMEM(phase_offset.shape, f32),
                pltpu.SMEM(order_gain.shape, f32),
                pltpu.SMEM(band_shift.shape, jnp.int32),
                pltpu.VMEM((phases, rows, pixels), bf16),
                pltpu.VMEM((2, half, 2 * wide), bf16),
                pltpu.VMEM(column.shape, bf16),
                pltpu.VMEM(inverse.shape, bf16),
                pltpu.VMEM(last.shape, bf16),
                pltpu.VMEM((8, 128), f32),
                pltpu.VMEM((count, 8, 128), f32),
                pltpu.VMEM((2, phases, CORES * rows, half), f32),
                pltpu.VMEM((phases // 2, 2, CORES * rows, half), f32),
                pltpu.VMEM((2, phases * CORES * rows, half), bf16),
                pltpu.VMEM((2, CORES * rows, tiles * wide), bf16),
                pltpu.VMEM((pixels, tiles * wide), f32),
                pltpu.VMEM((CORES * rows, 4 * wide), f32),
                pltpu.VMEM((CORES * rows, wide), f32),
                pltpu.VMEM((chips, CORES * rows, wide), f32),
                pltpu.VMEM((pixels, 4 * wide), f32),
                pltpu.VMEM((2, 4, phases, half, wide), f32),
                pltpu.VMEM((2, 2, 2, 2, half, 2 * wide), bf16),
                pltpu.VMEM((2, 2, rows, 2 * wide), f32),
                pltpu.VMEM((CORES, 2, 2, rows, 2 * wide), f32),
                pltpu.VMEM((chips, 2, CORES * rows, 2 * wide), f32),
                pltpu.VMEM((chips, CORES, 2, rows, 2 * wide), f32),
                pltpu.VMEM((chips, CORES, 2, packed, 2 * wide), f32),
                pltpu.VMEM((chips, CORES, 2, packed, 2 * wide), f32),
                pltpu.VMEM((2, rows, 2 * pixels), f32),
                pltpu.VMEM((2 * pixels // 128, 2 * rows, 128), f32),
                dma((chips,)), dma((chips,)),
                dma((3,)), dma((phases,)), dma((4,)),
                dma((count,)), dma((count,)),
                dma((2,)), dma((2,)),
                dma((2, 2)), dma((2, 2)),
                dma((chips, CORES, 2)), dma((chips, CORES, 2)),
                dma((chips, CORES, 2)), dma((chips, CORES, 2)),
            ],
            compiler_params=pltpu.CompilerParams(
                collective_id=0, has_side_effects=True, vmem_limit_bytes=60000000
            ),
        )(frames, phase_offset, order_gain, band_shift,
          jnp.asarray(lead), jnp.asarray(column), jnp.asarray(inverse), jnp.asarray(last))

    in_specs = (P("fov", None, "row", None), P("fov"), P("fov", None), P("fov", None))
    return jax.shard_map(
        per_device, mesh=mesh, in_specs=in_specs, out_specs=P(("fov", "row"), None), check_vma=False
    )
```

```python
import functools
import math

import jax
import jax.numpy as jnp
import numpy as np
from jax import lax
from jax.experimental import pallas as pl
from jax.experimental.pallas import tpu as pltpu
from jax.sharding import PartitionSpec as P

MESH = pl.DeviceIdType.MESH
wiener = 0.1
gain_out = 8.0
cut_share = 0.45
CORES = 2
STEP = 16


def max_shift(pixels):
    return 3 * pixels // 16


def split_table(table):
    high = table.astype(np.float32).astype(jnp.bfloat16)
    low = (table - high.astype(np.float64)).astype(np.float32).astype(jnp.bfloat16)
    return np.stack([high, low])


def cos_sin(points, freqs, length):
    angle = 2.0 * math.pi * ((points[:, None] * freqs[None, :]) % length) / length
    return np.cos(angle), np.sin(angle)


def limits(pixels, orders):
    lone, first = [math.ceil((pixels - cut_share * pixels - k * max_shift(pixels)) / CORES) - 1
                   for k in (orders - 1, orders)]
    wide = pixels // 2 // CORES
    return max(lone, wide - wide // 4), lone, first


def lane_order(wide, drop):
    return np.concatenate([np.arange(1, drop + 1), [0], np.arange(drop + 1, wide)])


def tables(pixels, count, orders):
    half = pixels // 2
    wide = half // CORES
    chips = count // CORES
    drop, lone, first = limits(pixels, orders)
    points = np.arange(pixels)
    freqs = np.arange(half)
    alternate = 1.0 - 2.0 * (points % 2)
    cos_f, sin_f = cos_sin(points, freqs, pixels)
    sin_f[:, 0] = alternate
    parities = [np.arange(q, half, 2) for q in range(2)]
    order = np.concatenate(parities)
    column = np.concatenate([cos_f[:, order], sin_f[:, order]], axis=1).T
    column = column.reshape(pixels, chips, pixels // chips).transpose(1, 0, 2)
    inverse = []
    for odd in range(2):
        cos_i, sin_i = cos_sin(2 * points[:half] + odd, freqs, 2 * pixels)
        sin_i[:, 0] = alternate[:half]
        inverse.append(np.stack([np.concatenate([cos_i[:, q], sin_i[:, q]], axis=1) for q in parities]))
    inverse = np.stack(inverse)
    lead, last = [], []
    places = np.arange(pixels)
    for core in range(CORES):
        own = CORES * lane_order(wide, drop) + core
        lead.append(np.concatenate([cos_f[:half, own], sin_f[:half, own]], axis=1))
        near_cos, near_sin = cos_sin(places, own, 2 * pixels)
        share = np.where(own == 0, 1.0, 2.0)
        near = np.concatenate([(near_cos * share).T, (-near_sin * share).T])
        mirror = np.where(own == 0, half, pixels - own)
        assert (pixels - own[:lone]).min() > cut_share * pixels + (orders - 1) * max_shift(pixels)
        assert (pixels - own[:first]).min() > cut_share * pixels + orders * max_shift(pixels)
        far_cos, far_sin = cos_sin(places, mirror, 2 * pixels)
        far = np.concatenate([(far_cos * 2.0).T, (-far_sin * 2.0).T])
        last.append(np.stack([near, far]))
    return tuple(split_table(t) for t in (np.stack(lead), column, inverse, np.stack(last)))


def otf_polynomial():
    nodes = 0.5 + 0.5 * np.cos(math.pi * (np.arange(64) + 0.5) / 64)
    nodes = np.minimum(nodes, 0.9985)
    values = 2 / math.pi * (np.arccos(nodes) - nodes * np.sqrt(1 - nodes * nodes)) / (1 - nodes) ** 1.5
    fit = np.polynomial.chebyshev.Chebyshev.fit(nodes, values, 6, domain=[0, 1])
    poly = fit.convert(kind=np.polynomial.Polynomial).coef
    return [float(c) for c in poly[::-1]]


def halves(value):
    high = value.astype(jnp.bfloat16)
    return high, (value - high.astype(jnp.float32)).astype(jnp.bfloat16)


def dot(left, right):
    return jnp.dot(left, right, preferred_element_type=jnp.float32)


def dot3(left_hi, left_lo, right_hi, right_lo):
    return dot(left_hi, right_hi) + (dot(left_hi, right_lo) + dot(left_lo, right_hi))


def kernel(count, poly, frames_h, offset_h, gain_h, shift_h, lead_h, column_h, inverse_h, last_h, out,
           offset, gain, shift, frames, lead, column, inverse, last, tot_send, tot, folds, ramps, planes, spec, mixed, outer_send, outer_recv, mixed_outer, alpha, coef,
           near_send, near, send_a, recv_a, send_b, recv_b, part, woven,
           outer_ss, outer_rs, small_sem, frame_sem, table_sem, tot_ss, tot_rs, fold_ss, fold_rs, near_ss, near_rs, a_ss, a_rs, b_ss, b_rs):
    me = lax.axis_index("row")
    chips = count // CORES
    chip, core = me // CORES, me % CORES
    sib_core = 1 - core
    phases, rows, pixels = frames.shape
    half = pixels // 2
    wide = half // CORES
    orders = phases // 2
    drop, lone, first_outer = limits(pixels, orders)
    turn_outer, pair = drop - first_outer, drop - lone
    mid = phases // 2
    others = [lax.rem(me + step, count) for step in range(1, count)]
    far_chips = [lax.rem(chip + step, chips) for step in range(1, chips)]
    sibling = chip * CORES + sib_core

    barrier = pltpu.get_barrier_semaphore()
    for peer in others:
        pl.semaphore_signal(barrier, inc=1, device_id={"row": peer}, device_id_type=MESH)
    frame_loads = []
    for p in range(phases):
        frame_loads.append(pltpu.make_async_copy(frames_h.at[0, p], frames.at[p], frame_sem.at[p]))
        frame_loads[p].start()
    small = []
    for idx, (source, target) in enumerate(((offset_h, offset), (gain_h, gain), (shift_h, shift))):
        small.append(pltpu.make_async_copy(source, target, small_sem.at[idx]))
        small[idx].start()
    loads = []
    for idx, (source, target) in enumerate(
        ((lead_h.at[:, core], lead), (column_h, column), (inverse_h, inverse), (last_h, last))
    ):
        loads.append(pltpu.make_async_copy(source, target, table_sem.at[idx]))
    loads[0].start()

    mine = pl.ds(pl.multiple_of(core * rows, rows), rows)
    lane8 = lax.broadcasted_iota(jnp.int32, (8, 128), 1)
    total_part = jnp.zeros((8, 128), jnp.float32)
    for p in range(phases):
        frame_loads[p].wait()
        lower, upper = frames[p, :, :half].astype(jnp.float32), frames[p, :, half:].astype(jnp.float32)
        both = lower + upper
        folds[0, p, mine, :] = both
        folds[1, p, mine, :] = lower - upper
        s = jnp.sum(jnp.sum(both, axis=0, keepdims=True), axis=1, keepdims=True)
        total_part = total_part + jnp.where(lane8 == p, s, 0.0)
    tot_send[...] = total_part
    tot[me] = total_part
    pl.semaphore_wait(barrier, count - 1)

    def tot_copy(peer, slot):
        return pltpu.make_async_remote_copy(
            src_ref=tot_send, dst_ref=tot.at[slot], send_sem=tot_ss.at[peer], recv_sem=tot_rs.at[slot],
            device_id={"row": peer}, device_id_type=MESH)

    for peer in others:
        tot_copy(peer, me).start()

    def fold_copy(slot_core, k):
        place = pl.ds(pl.multiple_of(slot_core * rows, rows), rows)
        return pltpu.make_async_remote_copy(
            src_ref=folds.at[k, :, place], dst_ref=folds.at[k, :, place],
            send_sem=fold_ss.at[k], recv_sem=fold_rs.at[k],
            device_id={"row": sibling}, device_id_type=MESH)

    for k in range(2):
        fold_copy(core, k).start()
    for load in loads[1:]:
        load.start()

    for load in small:
        load.wait()
    shift_y, shift_x = shift[0, 0], shift[0, 1]
    inv_cut = 1.0 / (cut_share * pixels)
    scale_out = 0.5 * gain_out / (4.0 * pixels * pixels)
    gains = [gain[0, j] for j in range(phases)]
    squares = [g * g for g in gains]
    scaled = [g * scale_out for g in gains]
    reach = int(cut_share * pixels) + 1 + 2 * max_shift(pixels)
    single = max((pixels - reach) // 2 // STEP, 1)
    quarter = half // 2

    def blocks(block, few, many):
        for odd in range(2):
            def body(which, i, carry):
                block(pl.multiple_of(i * STEP, STEP), odd, which, False)
                return carry

            lax.fori_loop(1 - odd, single, functools.partial(body, few), 0)
            lax.fori_loop(single, quarter // STEP, functools.partial(body, many), 0)

    def own_freq(shape):
        lane = lax.broadcasted_iota(jnp.int32, shape, 1)
        place = jnp.where(lane < drop, lane + 1, jnp.where(lane == drop, 0, lane))
        return CORES * place + core

    def make_alpha(side):
        freq = own_freq((STEP, wide))
        if side:
            freq = jnp.where(freq == 0, half, pixels - freq)
        used = [j for j in range(phases) if not (side and j == mid)]
        sq_xs = {}
        for j in used:
            fx = (freq - (j - mid) * shift_x).astype(jnp.float32) * inv_cut
            sq_xs[j] = fx * fx + 1e-30
        offs = {j: ((j - mid) * shift_y).astype(jnp.float32) * inv_cut for j in used}

        def block(first, odd, slots, top):
            row = 2 * (first + lax.broadcasted_iota(jnp.int32, (STEP, wide), 0)) + odd
            here = pl.ds(odd * quarter + first, STEP)
            for slot in slots:
                big_y = row if slot % 2 == 0 else -row
                if top and slot % 2:
                    big_y = jnp.where(row == 0, -half, big_y)
                if slot == 2:
                    big_y = big_y - pixels
                if slot == 3:
                    big_y = big_y + pixels
                unit_y = big_y.astype(jnp.float32) * inv_cut
                den = jnp.full((STEP, wide), wiener, jnp.float32)
                den_m = jnp.full((STEP, wide), wiener, jnp.float32)
                values = {}
                for j in used:
                    fy = unit_y - offs[j]
                    t = fy * fy + sq_xs[j]
                    r = t * lax.rsqrt(t)
                    u = jnp.maximum(1.0 - r, 1e-30)
                    v = u * lax.rsqrt(u)
                    acc = poly[0] * r + poly[1]
                    for c in poly[2:]:
                        acc = acc * r + c
                    value = acc * (u * v)
                    values[j] = value
                    sq = value * value
                    den = den + squares[j] * sq
                    den_m = den_m + squares[phases - 1 - j] * sq
                both = 1.0 / (den * den_m)
                inv, inv_m = den_m * both, den * both
                for j in used:
                    alpha[side, slot, j, here, :] = values[j] * (
                        scaled[j] * inv + scaled[phases - 1 - j] * inv_m)

        block(0, 0, (0, 1, 2, 3), True)
        blocks(block, (0, 1), (0, 1, 2, 3))

    turn = 2.0 * math.pi / pixels

    def ramp(points, step):
        arg = ((points * step) & (pixels - 1)).astype(jnp.float32) * turn
        return jnp.cos(arg), jnp.sin(arg)

    def times(left, right):
        return left[0] * right[0] - left[1] * right[1], left[0] * right[1] + left[1] * right[0]

    row8 = lax.broadcasted_iota(jnp.int32, (8, 128), 0) + chip * (CORES * rows)
    wave_x = [ramp(lane8 + 128 * k, shift_x) for k in range(half // 128)]
    base = ramp(row8, shift_y)
    leap = ramp(jnp.full((8, 128), 8, jnp.int32), shift_y)
    pieces = [base]
    for k in range(1, CORES * rows // 8):
        pieces.append(times(pieces[-1], leap))
    wave_y = tuple(jnp.concatenate([q[k] for q in pieces], axis=0) for k in range(2))
    start = jnp.full((8, 128), offset[0], jnp.float32)
    wave_x = [times(w, (jnp.cos(start), -jnp.sin(start))) for w in wave_x]
    for k in range(half // 128):
        turned = times(wave_y, (wave_x[k][0][:1], wave_x[k][1][:1]))
        value = turned
        for order in range(orders):
            if order:
                value = times(value, turned)
            for q in range(2):
                ramps[order, q, :, pl.ds(k * 128, 128)] = value[q]

    make_alpha(0)

    for peer in others:
        tot_copy(peer, peer).wait_recv()
    total = tot[0]
    for d in range(1, count):
        total = total + tot[d]
    level = jnp.where(lane8 < phases, float(pixels * pixels), 0.0) / jnp.where(lane8 < phases, total, 1.0)
    level = level / phases

    groups = [(4 * g, 4, g + 1) for g in range(orders)] + [(4 * orders, 2, 0)]

    span_rows = CORES * rows

    def scaled_folds(which, rows_at, lanes_at):
        return [level[:1, p:p + 1] * folds[which, p, rows_at, lanes_at] for p in range(phases)]

    def modulated(order, values, rows_at, lanes_at):
        re, im = values[0], None
        for q in range(1, mid + 1):
            theta = 2.0 * math.pi * order * q / phases
            re = re + math.cos(theta) * (values[q] + values[phases - q])
            term = -math.sin(theta) * (values[q] - values[phases - q])
            im = term if im is None else im + term
        return times((re, im), [ramps[order - 1, k, rows_at, lanes_at] for k in range(2)])

    swapped = core + (shift_x & 1) * (1 - 2 * core)

    def unmix(wanted):
        which = swapped if wanted[0] % 2 else core
        for r in range(0, span_rows, STEP):
            for x in range(0, half, 128):
                rows_at, lanes_at = pl.ds(r, STEP), pl.ds(x, 128)
                values = scaled_folds(which, rows_at, lanes_at)
                for order in wanted:
                    if order:
                        made = modulated(order, values, rows_at, lanes_at)
                    else:
                        made = [functools.reduce(lambda a, b: a + b, values)]
                    for k, value in enumerate(made):
                        hi, lo = halves(value)
                        place = 2 * (order - 1) * span_rows + 2 * r + k * STEP if order else 2 * orders * span_rows + r
                        planes[0, pl.ds(place, STEP), lanes_at] = hi
                        planes[1, pl.ds(place, STEP), lanes_at] = lo

    forward = shift_x >= 0
    free = first_outer + 2 * turn_outer - wide

    def outer_copy(c, slot_chip):
        return pltpu.make_async_remote_copy(
            src_ref=outer_send, dst_ref=outer_recv.at[slot_chip],
            send_sem=outer_ss.at[c], recv_sem=outer_rs.at[slot_chip],
            device_id={"row": c * CORES + core}, device_id_type=MESH)

    def spectrum(g):
        first, tiles, order = groups[g]
        place = 2 * (order - 1) if order else 2 * orders
        span = pl.ds(place * span_rows, (2 if order else 1) * span_rows)
        result = dot3(planes[0, span, :], planes[1, span, :], lead[0], lead[1])
        special = jnp.logical_and(lax.broadcasted_iota(jnp.int32, (STEP, wide), 1) == drop, core == 0)
        for r in range(0, span_rows, STEP):
            if order:
                re, im = result[2 * r:2 * r + STEP], result[2 * r + STEP:2 * r + 2 * STEP]
                cr, sr, ci, si = re[:, :wide], re[:, wide:], im[:, :wide], im[:, wide:]
                values = [jnp.where(special, cr, cr + si), jnp.where(special, ci, ci - sr),
                          jnp.where(special, sr, cr - si), jnp.where(special, si, ci + sr)]
            else:
                re = result[r:r + STEP]
                values = [re[:, :wide], jnp.where(special, 0.0, -re[:, wide:])]
            for k, value in enumerate(values):
                hi, lo = halves(value)
                spec[0, pl.ds(r, STEP), pl.ds((first + k) * wide, wide)] = hi
                spec[1, pl.ds(r, STEP), pl.ds((first + k) * wide, wide)] = lo
            if order >= orders - 1:
                outer_re = jnp.where(forward, values[2], values[0])
                outer_im = jnp.where(forward, values[3], -values[1])
                lane = lax.broadcasted_iota(jnp.int32, (STEP, wide), 1)
                if order == orders:
                    here = jnp.logical_and(lane >= first_outer, lane < drop)
                    full = jnp.where(here, outer_re, pltpu.roll(outer_im, turn_outer, 1))
                    below = jnp.logical_and(lane >= free, lane < free + 2 * pair)
                    outer_send[pl.ds(r, STEP), :] = jnp.where(below, outer_send[pl.ds(r, STEP), :], full)
                else:
                    outer_send[pl.ds(r, STEP), :] = jnp.where(
                        lane < free + pair, pltpu.roll(outer_re, wide - (lone - free), 1),
                        pltpu.roll(outer_im, wide - (lone - free - pair), 1))

    loads[0].wait()
    for k in range(2):
        fold_copy(sib_core, k).wait_recv()
    for order in range(1, orders + 1, 2):
        unmix([order])
        spectrum(order - 1)
    unmix(list(range(2, orders + 1, 2)) + [0])
    for order in range(2, orders + 1, 2):
        spectrum(order - 1)
    for c in far_chips:
        outer_copy(c, chip).start()
    spectrum(orders)
    loads[1].wait()
    for first, tiles, _ in groups:
        window = pl.ds(first * wide, tiles * wide)
        mixed[:, window] = dot3(column[0, chip], column[1, chip], spec[0, :, window], spec[1, :, window])

    special = jnp.logical_and(lax.broadcasted_iota(jnp.int32, (STEP, wide), 1) == drop, core == 0)

    outer_lanes = lax.broadcasted_iota(jnp.int32, (STEP, wide), 1) < drop

    def combine(side):
        def block(first, odd, second, top):
            here, below = pl.ds(odd * quarter + first, STEP), pl.ds(half + odd * quarter + first, STEP)
            upper, lower = pl.ds(first, STEP), pl.ds(quarter + first, STEP)
            row0 = None
            if top:
                row0 = lax.broadcasted_iota(jnp.int32, (STEP, wide), 0) == 0

            def pick(at_top, value):
                return jnp.where(row0, at_top, value) if top else value

            def signs(tile, source=mixed):
                re, im = pl.ds(tile * wide, wide), pl.ds((tile + 1) * wide, wide)
                cr, ci, sr, si = source[here, re], source[here, im], source[below, re], source[below, im]
                plus = (pick(cr, cr + si), pick(ci, ci - sr))
                minus = (pick(sr, cr - si), pick(si, ci + sr))
                return plus, minus

            slots = (0, 1, 2, 3) if second else (0, 1)
            sums = {slot: [None, None] for slot in slots}

            def add(slot, k, term):
                sums[slot][k] = term if sums[slot][k] is None else sums[slot][k] + term

            if side == 0:
                center = signs(4 * orders)
                for slot in slots:
                    a = alpha[side, slot, mid, here, :]
                    for k in range(2):
                        add(slot, k, a * center[slot % 2][k])
            for order in range(1, orders + 1):
                pos, neg = signs(4 * (order - 1)), signs(4 * (order - 1) + 2)
                direct, other = (pos, neg) if side == 0 else (neg, pos)
                partner = [[jnp.where(special, direct[s][k], other[s][k]) for k in range(2)] for s in range(2)]
                if top:
                    swap = [[pick(partner[s][k], partner[1 - s][k]) for k in range(2)] for s in range(2)]
                else:
                    swap = [partner[1], partner[0]]
                for slot in slots:
                    s = slot % 2
                    up, down = alpha[side, slot, mid + order, here, :], alpha[side, slot, mid - order, here, :]
                    add(slot, 0, up * direct[s][0] + down * swap[s][0])
                    add(slot, 1, up * direct[s][1] - down * swap[s][1])
            if side:
                outer_parts = [(orders - q, signs(2 * q, mixed_outer)) for q in range(2)]
                for slot in slots:
                    weights = [jnp.where(forward, alpha[side, slot, mid + order, here, :],
                                         alpha[side, slot, mid - order, here, :]) for order, _ in outer_parts]
                    for k in range(2):
                        whole = weights[0] * outer_parts[0][1][slot % 2][k] + weights[1] * outer_parts[1][1][slot % 2][k]
                        sums[slot][k] = jnp.where(outer_lanes, whole, sums[slot][k])
            for a in range(2):
                def folded(s, k):
                    if not second:
                        return sums[s][k]
                    return sums[s][k] + sums[2 + s][k] if a == 0 else sums[s][k] - sums[2 + s][k]

                pr, pi, mr, mi = folded(0, 0), folded(0, 1), folded(1, 0), folded(1, 1)
                low_top = (mr, mi) if a == 0 else (mi, -mr)
                values = [(upper, 0, pick(pr, pr + mr)), (upper, 1, pick(pi, pi + mi)),
                          (lower, 0, pick(low_top[0], mi - pi)), (lower, 1, pick(low_top[1], pr - mr))]
                for place, k, value in values:
                    hi, lo = halves(value)
                    coef[0, side, a, odd, place, pl.ds(k * wide, wide)] = hi
                    coef[1, side, a, odd, place, pl.ds(k * wide, wide)] = lo

        block(0, 0, True, True)
        blocks(block, False, True)

    flip = jnp.where(chip == 0, 1.0, -1.0)

    def to_rows(side, a):
        even, odd = [dot3(inverse[0, a, q], inverse[1, a, q], coef[0, side, a, q], coef[1, side, a, q])
                     for q in range(2)]
        odd = odd * flip
        return even + odd, even - odd

    def keep_near(side, a, value):
        first, second = value[:rows], value[rows:]
        near[core, side, a] = jnp.where(core == 0, first, second)
        near_send[side, a] = jnp.where(core == 0, second, first)
        near_copy(core, side, a).start()

    def a_copy(c, kc, slot_chip, slot_core, a):
        return pltpu.make_async_remote_copy(
            src_ref=send_a.at[c, a, pl.ds(pl.multiple_of(kc * rows, rows), rows), :], dst_ref=recv_a.at[slot_chip, slot_core, a],
            send_sem=a_ss.at[c, kc, a], recv_sem=a_rs.at[slot_chip, slot_core, a],
            device_id={"row": c * CORES + kc}, device_id_type=MESH)

    def b_copy(c, kc, slot_chip, slot_core, a):
        return pltpu.make_async_remote_copy(
            src_ref=send_b.at[c, kc, a], dst_ref=recv_b.at[slot_chip, slot_core, a],
            send_sem=b_ss.at[c, kc, a], recv_sem=b_rs.at[slot_chip, slot_core, a],
            device_id={"row": c * CORES + kc}, device_id_type=MESH)

    def near_copy(slot_core, side, a):
        return pltpu.make_async_remote_copy(
            src_ref=near_send.at[side, a], dst_ref=near.at[slot_core, side, a],
            send_sem=near_ss.at[side, a], recv_sem=near_rs.at[side, a],
            device_id={"row": sibling}, device_id_type=MESH)

    combine(0)
    loads[2].wait()
    for c in far_chips:
        for a in range(2):
            own_rows, far_rows = to_rows(0, a)
            send_a[c, a] = far_rows
            for kc in (core, sib_core):
                a_copy(c, kc, chip, core, a).start()
            keep_near(0, a, own_rows)

    make_alpha(1)
    own = [[], []]
    for order in (orders, orders - 1):
        tiles = [pl.ds((4 * (order - 1) + k) * wide, wide) for k in range(4)]
        for part_at in range(2):
            plus_re, plus_im, minus_re, minus_im = [spec[part_at, :, t].astype(jnp.float32) for t in tiles]
            own[part_at].append(jnp.where(forward, minus_re, plus_re).astype(jnp.bfloat16))
            own[part_at].append(jnp.where(forward, minus_im, -plus_im).astype(jnp.bfloat16))
    hi, lo = [jnp.concatenate(value, axis=1) for value in own]
    mixed_outer[...] = dot3(column[0, chip], column[1, chip], hi, lo)
    for c in far_chips:
        outer_copy(c, c).wait_recv()
        tile = outer_recv[c]
        hi, lo = halves(jnp.concatenate([tile, pltpu.roll(tile, wide - turn_outer, 1), pltpu.roll(tile, lone - free, 1),
                                         pltpu.roll(tile, lone - free - pair, 1)], axis=1))
        mixed_outer[...] += dot3(column[0, c], column[1, c], hi, lo)
    combine(1)
    packed = send_b.shape[3]
    shared = rows // packed
    kept = wide - drop
    lane_t = lax.broadcasted_iota(jnp.int32, (packed, wide), 1)
    kept_lanes = lax.broadcasted_iota(jnp.int32, (rows, wide), 1) >= drop
    for c in far_chips:
        for a in range(2):
            own_rows, far_rows = to_rows(1, a)
            for kc in range(CORES):
                for k in range(2):
                    piece = far_rows[kc * rows:(kc + 1) * rows, k * wide:(k + 1) * wide]
                    lanes = pl.ds(k * wide, wide)
                    value = piece[:packed]
                    for i in range(1, shared):
                        moved = pltpu.roll(piece[i * packed:(i + 1) * packed], wide - i * kept, 1)
                        value = jnp.where(lane_t < wide - i * kept, moved, value)
                    send_b[c, kc, a, :, lanes] = value
            for kc in (core, sib_core):
                b_copy(c, kc, chip, core, a).start()
            keep_near(1, a, own_rows)

    loads[3].wait()
    chunk = 256
    for side in range(2):
        for a in range(2):
            near_copy(sib_core, side, a).wait_recv()

    def finish(a, side, pieces, write):
        split = [halves(piece) for piece in pieces]
        for x in range(0, pixels, chunk):
            span = pl.ds(x, chunk)
            even, odd = [dot3(hi, lo, last[0, k, side, :, span], last[1, k, side, :, span])
                         for k, (hi, lo) in enumerate(split)]
            write(a, x, even + odd)
            write(a, pixels + x, even - odd)

    def write_part(a, x, value):
        part[a, :, pl.ds(x, chunk)] = value

    for a in range(2):
        pieces = []
        for k in range(CORES):
            value = near[k, 0, a]
            for c in far_chips:
                a_copy(c, k, c, k, a).wait_recv()
                value = value + recv_a[c, k, a]
            pieces.append(value)
        finish(a, 0, pieces, write_part)

    def unpacked(c, k, a):
        sides = []
        for q in range(2):
            lanes = pl.ds(q * wide, wide)
            value = recv_b[c, k, a, :, lanes]
            joined = jnp.concatenate([value] + [pltpu.roll(value, i * kept, 1) for i in range(1, shared)], axis=0)
            sides.append(jnp.where(kept_lanes, joined, 0.0))
        return jnp.concatenate(sides, axis=1)

    for a in range(2):
        for k in (core, sib_core):
            sign = jnp.where(k == 0, 1.0, -1.0)
            value = near[k, 1, a]
            for c in far_chips:
                b_copy(c, k, c, k, a).wait_recv()
                value = value + unpacked(c, k, a)
            hi, lo = halves(value)
            for x in range(0, pixels, chunk):
                span = pl.ds(x, chunk)
                value = dot3(hi, lo, last[0, k, 1, :, span], last[1, k, 1, :, span])
                for at, term in ((x, value), (pixels + x, sign * value)):
                    total = part[a, :, pl.ds(at, chunk)] + term
                    if k is core:
                        part[a, :, pl.ds(at, chunk)] = total
                        continue
                    for q in range(chunk // 128):
                        tile = at // 128 + q
                        woven[tile, pl.ds(a, rows, stride=2), :] = total[:, q * 128:(q + 1) * 128]
                        if a:
                            out[:, pl.ds(tile * 128, 128)] = woven[tile]

    for peer in others:
        tot_copy(peer, me).wait_send()
    for k in range(2):
        fold_copy(core, k).wait_send()
    for c in far_chips:
        outer_copy(c, chip).wait_send()
    for a in range(2):
        for side in range(2):
            near_copy(core, side, a).wait_send()
        for c in far_chips:
            for kc in range(CORES):
                a_copy(c, kc, chip, core, a).wait_send()
                b_copy(c, kc, chip, core, a).wait_send()


def solution(mesh):
    count = mesh.shape["row"]

    def per_device(frames, phase_offset, order_gain, band_shift):
        phases, rows, pixels = frames.shape[1:]
        chips = count // CORES
        assert chips == 2 and CORES == 2
        half = pixels // 2
        wide = half // CORES
        tiles = 4 * (phases // 2) + 2
        packed = rows // 4
        orders = phases // 2
        drop, lone, first = limits(pixels, orders)
        assert 4 * (wide - drop) <= wide and 2 * (drop - first) + 2 * (drop - lone) <= wide < 2 * drop
        lead, column, inverse, last = tables(pixels, count, orders)
        vmem = pl.BlockSpec(memory_space=pltpu.VMEM)
        hbm = pl.BlockSpec(memory_space=pl.ANY)
        bf16, f32 = jnp.bfloat16, jnp.float32
        dma = pltpu.SemaphoreType.DMA
        return pl.pallas_call(
            functools.partial(kernel, count, otf_polynomial()),
            out_shape=pltpu.VMEM((2 * rows, 2 * pixels), f32),
            in_specs=[hbm] * 8,
            out_specs=vmem,
            scratch_shapes=[
                pltpu.SMEM(phase_offset.shape, f32),
                pltpu.SMEM(order_gain.shape, f32),
                pltpu.SMEM(band_shift.shape, jnp.int32),
                pltpu.VMEM((phases, rows, pixels), bf16),
                pltpu.VMEM((2, half, 2 * wide), bf16),
                pltpu.VMEM(column.shape, bf16),
                pltpu.VMEM(inverse.shape, bf16),
                pltpu.VMEM(last.shape, bf16),
                pltpu.VMEM((8, 128), f32),
                pltpu.VMEM((count, 8, 128), f32),
                pltpu.VMEM((2, phases, CORES * rows, half), f32),
                pltpu.VMEM((phases // 2, 2, CORES * rows, half), f32),
                pltpu.VMEM((2, phases * CORES * rows, half), bf16),
                pltpu.VMEM((2, CORES * rows, tiles * wide), bf16),
                pltpu.VMEM((pixels, tiles * wide), f32),
                pltpu.VMEM((CORES * rows, wide), f32),
                pltpu.VMEM((chips, CORES * rows, wide), f32),
                pltpu.VMEM((pixels, 4 * wide), f32),
                pltpu.VMEM((2, 4, phases, half, wide), f32),
                pltpu.VMEM((2, 2, 2, 2, half, 2 * wide), bf16),
                pltpu.VMEM((2, 2, rows, 2 * wide), f32),
                pltpu.VMEM((CORES, 2, 2, rows, 2 * wide), f32),
                pltpu.VMEM((chips, 2, CORES * rows, 2 * wide), f32),
                pltpu.VMEM((chips, CORES, 2, rows, 2 * wide), f32),
                pltpu.VMEM((chips, CORES, 2, packed, 2 * wide), f32),
                pltpu.VMEM((chips, CORES, 2, packed, 2 * wide), f32),
                pltpu.VMEM((2, rows, 2 * pixels), f32),
                pltpu.VMEM((2 * pixels // 128, 2 * rows, 128), f32),
                dma((chips,)), dma((chips,)),
                dma((3,)), dma((phases,)), dma((4,)),
                dma((count,)), dma((count,)),
                dma((2,)), dma((2,)),
                dma((2, 2)), dma((2, 2)),
                dma((chips, CORES, 2)), dma((chips, CORES, 2)),
                dma((chips, CORES, 2)), dma((chips, CORES, 2)),
            ],
            compiler_params=pltpu.CompilerParams(
                collective_id=0, has_side_effects=True, vmem_limit_bytes=60000000
            ),
        )(frames, phase_offset, order_gain, band_shift,
          jnp.asarray(lead), jnp.asarray(column), jnp.asarray(inverse), jnp.asarray(last))

    in_specs = (P("fov", None, "row", None), P("fov"), P("fov", None), P("fov", None))
    return jax.shard_map(
        per_device, mesh=mesh, in_specs=in_specs, out_specs=P(("fov", "row"), None), check_vma=False
    )
```
